8 devices in a mesh: ens: 2 (over z, y), feat: 4 (over x, core).
Axes of the slice: x: 2, y: 2, z: 1, core: 2. Of those that a mesh axis runs over, the one named last changes fastest.
Arguments:
- particles: float32 [4, 512, 16384], P('ens', None, 'feat'), parts along dimension 0
- target_mean: float32 [4, 16384], P('ens', 'feat'), parts along dimension 0
- precision: float32 [32768], P(('ens', 'feat')), parts along dimension 0
- low_factor: bfloat16 [32768, 128], P(('ens', 'feat')), parts along dimension 0
Outputs:
- output: float32 [4, 512, 16384], P('ens', None, 'feat'), parts along dimension 0
There are 2 independent parts. The reference program is written for one: setup_inputs(seed, part) draws one part's arguments, and reference() takes and returns one part's arrays. A program takes and returns all parts, laid end to end along the dimension named above; each array names one.
All inputs are finite; a program needn't handle non-finite values.
Results may differ from the reference program's by a relative error of at most 0.001.
Values are sent between devices in bfloat16 or wider.
A program may use at most 1 GiB of HBM per device.

```python
import jax
import jax.numpy as jnp
from jax import lax

PARTICLES = 512
FEATURES = 16384
LOW_RANK = 128
NUM_STEPS = 3


def setup_inputs(seed: int = 0, part: int = 0) -> dict:
    base_key = jax.random.fold_in(jax.random.key(seed), part)
    key_list = jax.random.split(base_key, 7)
    prec_scale = 2.0 / FEATURES
    factor_scale = prec_scale ** 0.5 / FEATURES ** 0.5
    low_raw = factor_scale * jax.random.normal(key_list[0], (FEATURES, LOW_RANK), jnp.float32)
    precision = prec_scale * jax.random.uniform(key_list[1], (FEATURES,), jnp.float32, 0.5, 1.5)
    target_mean = jax.random.normal(key_list[2], (2, FEATURES), jnp.float32)
    center = 0.7 * jax.random.normal(key_list[3], (2, FEATURES), jnp.float32)
    coef_vec = jax.random.normal(key_list[4], (2, LOW_RANK), jnp.float32)
    aligned = jnp.dot(coef_vec, low_raw.T) * (0.7 / (factor_scale * LOW_RANK ** 0.5))
    spread = jax.random.uniform(key_list[5], (2, PARTICLES, 1), jnp.float32, 0.5, 1.5)
    noise_mat = jax.random.normal(key_list[6], (2, PARTICLES, FEATURES), jnp.float32)
    particles = (target_mean + center + aligned)[:, None, :] + spread * noise_mat
    return {"particles": particles, "target_mean": target_mean, "precision": precision, "low_factor": low_raw.astype(jnp.bfloat16)}


def svgd_step(theta, target_mean, precision, low_factor):
    bandwidth = 2.0 * FEATURES
    step_size = 0.25 * FEATURES
    low_wide = low_factor.astype(jnp.float32)
    centered = theta - target_mean[:, None, :]
    project = jnp.einsum("end,dr->enr", centered.astype(jnp.bfloat16).astype(jnp.float32), low_wide)
    theta_wide = theta.astype(jnp.bfloat16).astype(jnp.float32)
    gram_mat = jnp.einsum("end,emd->enm", theta_wide, theta_wide)
    gram_diag = jnp.diagonal(gram_mat, axis1=1, axis2=2)
    sq_dist = jnp.maximum(gram_diag[:, :, None] + gram_diag[:, None, :] - 2.0 * gram_mat, 0.0)
    kernel = jnp.exp(-sq_dist / bandwidth)
    low_term = jnp.einsum("enr,dr->end", project.astype(jnp.bfloat16).astype(jnp.float32), low_wide)
    grad_log = -(centered * precision + low_term)
    mixed = (grad_log - (2.0 / bandwidth) * theta).astype(jnp.bfloat16).astype(jnp.float32)
    drive = jnp.einsum("enm,emd->end", kernel.astype(jnp.bfloat16).astype(jnp.float32), mixed)
    row_sum = jnp.sum(kernel, axis=2, keepdims=True)
    return theta + step_size * ((drive + (2.0 / bandwidth) * row_sum * theta) / PARTICLES)


def reference(particles, target_mean, precision, low_factor):
    def scan_body(theta, unused):
        return svgd_step(theta, target_mean, precision, low_factor), None
    final_theta, unused_out = lax.scan(scan_body, particles, None, length=NUM_STEPS)
    return final_theta
```

```python
import jax
import jax.numpy as jnp
from jax import lax
from jax.experimental import pallas as pl
from jax.experimental.pallas import tpu as pltpu
from jax.sharding import PartitionSpec as P

NUM_STEPS = 3
BLK = 128
TILE = 512
F32 = jnp.float32
BF16 = jnp.bfloat16
TRANS_B = (((1,), (1,)), ((), ()))

SEM_CORE, SEM_CHIP, SEM_GATHER, SEM_OWN, SEM_FWD = range(5)
NUM_KINDS = 3
NUM_SEMS = 5 * NUM_KINDS


def build_kernel(num_part, num_local, total_feat):
    nblk = num_part // BLK
    num_tiles = num_local // TILE
    bandwidth = 2.0 * total_feat
    step_size = 0.25 * total_feat
    two_h = 2.0 / bandwidth
    gain = step_size / num_part
    grow = 2 * BLK + BLK // 2

    def kernel(th_hbm, mu_ref, lam_ref, u_ref, out_hbm,
               theta, tb, kfull, qacc, scol,
               pq, pg, pd, rq, rg, rd, sq, sg, sd, xq, xg, xd, dfull, gsum,
               qall, kall, sall,
               in_sem, out_sem, send_sem, recv_sem):
        feat = lax.axis_index("feat")
        chip = feat // 2
        core = feat % 2
        own = 2 * core + chip
        peer_core = {"feat": 2 * chip + (1 - core)}
        peer_chip = {"feat": 2 * (1 - chip) + core}

        barrier = pltpu.get_barrier_semaphore()
        for peer in (peer_core, peer_chip):
            pl.semaphore_signal(barrier, inc=1, device_id=peer, device_id_type=pl.DeviceIdType.MESH)
        pl.semaphore_wait(barrier, 2)

        def rcopy(src, dst, e, group, kind, peer):
            idx = group * NUM_KINDS + kind
            return pltpu.make_async_remote_copy(
                src_ref=src, dst_ref=dst, send_sem=send_sem.at[e, idx], recv_sem=recv_sem.at[e, idx],
                device_id=peer, device_id_type=pl.DeviceIdType.MESH)

        def tile_ds(t):
            return pl.ds(pl.multiple_of(t * TILE, TILE), TILE)

        def in_copy(e, t):
            return pltpu.make_async_copy(th_hbm.at[e, :, tile_ds(t)], theta.at[e, :, tile_ds(t)], in_sem.at[e, t])

        def out_copy(e, t):
            return pltpu.make_async_copy(theta.at[e, :, tile_ds(t)], out_hbm.at[e, :, tile_ds(t)], out_sem.at[e, t])

        def core_q(e):
            return rcopy(pq.at[e, pl.ds(2 * (1 - core), 2)], rq.at[e], e, SEM_CORE, 0, peer_core)

        def core_g(e):
            return rcopy(pg.at[e, pl.ds(2 * (1 - core), 2)], rg.at[e], e, SEM_CORE, 1, peer_core)

        def core_d(e):
            return rcopy(pd.at[e], rd.at[e], e, SEM_CORE, 2, peer_core)

        def chip_q(e):
            return rcopy(sq.at[e, 1 - chip], xq.at[e], e, SEM_CHIP, 0, peer_chip)

        def chip_g(e):
            return rcopy(sg.at[e, 1 - chip], xg.at[e], e, SEM_CHIP, 1, peer_chip)

        def chip_d(e):
            return rcopy(sd.at[e], xd.at[e], e, SEM_CHIP, 2, peer_chip)

        def gather(e, slot, group, kind, peer):
            buf = (qall, kall, sall)[kind]
            if kind == 0:
                ref = buf.at[e, pl.ds(pl.multiple_of(slot * BLK, BLK), BLK)]
            else:
                ref = buf.at[e, slot]
            return rcopy(ref, ref, e, group, kind, peer)

        def to_chip(e, kind):
            return gather(e, own, SEM_GATHER, kind, peer_chip)

        def to_core(e, kind):
            return gather(e, own, SEM_OWN, kind, peer_core)

        def forward(e, kind):
            return gather(e, 2 * core + (1 - chip), SEM_FWD, kind, peer_core)

        def stage2_q(e):
            core_q(e).wait()
            for c in range(2):
                sq[e, c] = pq[e, 2 * core + c] + rq[e, c]
            chip_q(e).start()

        def stage2_g(e):
            core_g(e).wait()
            core_d(e).wait()
            sd[e] = pd[e] + rd[e]
            chip_d(e).start()
            for c in range(2):
                sg[e, c] = pg[e, 2 * core + c] + rg[e, c]
            chip_g(e).start()

        def stage3_q(e):
            chip_q(e).wait()
            full = sq[e, chip] + xq[e]
            qall[e, pl.ds(pl.multiple_of(own * BLK, BLK), BLK), :] = full.astype(BF16)
            to_chip(e, 0).start()
            to_core(e, 0).start()

        def stage3_g(e):
            chip_d(e).wait()
            chip_g(e).wait()
            dfull[...] = sd[e] + xd[e]
            gsum[...] = sg[e, chip] + xg[e]
            sall[e, own] = jnp.zeros((8, BLK), F32)
            wrap = own // 3
            half = own // 2
            parts = (
                (0, BLK, own, own, 0),
                (BLK, BLK, own - 3 * wrap, own + 1 - wrap, 0),
                (2 * BLK, BLK // 2, own % 2, own % 2 + 2, half * (BLK // 2)),
            )
            for index, (start, size, row_blk, col_blk, row_off) in enumerate(parts):
                row_id = lax.broadcasted_iota(jnp.int32, (size, BLK), 0) + row_off
                col_id = lax.broadcasted_iota(jnp.int32, (size, BLK), 1)
                eye = row_id == col_id
                diag_col = jnp.sum(jnp.where(eye, dfull[pl.ds(row_blk, 1), :], 0.0), axis=1, keepdims=True)
                diag_row = dfull[pl.ds(col_blk, 1), :]
                dist = jnp.maximum(diag_col + diag_row - 2.0 * gsum[start:start + size, :], 0.0)
                kern = jnp.exp(-dist / bandwidth)
                kall[e, own, start:start + size, :] = kern.astype(BF16)
                sall[e, own, pl.ds(col_blk, 1), :] += jnp.sum(kern, axis=0, keepdims=True)
                if index > 0:
                    row_sum = jnp.sum(kern, axis=1, keepdims=True)
                    sall[e, own, pl.ds(row_blk, 1), :] += jnp.sum(jnp.where(eye, row_sum, 0.0), axis=0, keepdims=True)
            for kind in (1, 2):
                to_chip(e, kind).start()
                to_core(e, kind).start()

        def stage4(e, kinds):
            for kind in kinds:
                to_chip(e, kind).wait()
                forward(e, kind).start()

        def stage5(e):
            for kind in range(NUM_KINDS):
                to_core(e, kind).wait()
                forward(e, kind).wait()
            half = BLK // 2

            def put(i, j, rows, block):
                r0 = i * BLK + rows
                n = block.shape[0]
                kfull[r0:r0 + n, j * BLK:(j + 1) * BLK] = block

            def put_pair(i, j, block):
                put(i, j, 0, block)
                put(j, i, 0, block.astype(F32).T.astype(BF16))

            for i in range(nblk):
                put(i, i, 0, kall[e, i, 0:BLK, :])
            for i, j, o in ((0, 1, 0), (1, 2, 1), (2, 3, 2), (0, 3, 3)):
                put_pair(i, j, kall[e, o, BLK:2 * BLK, :])
            for i in range(2):
                lo = kall[e, i, 2 * BLK:2 * BLK + half, :]
                hi = kall[e, i + 2, 2 * BLK:2 * BLK + half, :]
                put_pair(i, i + 2, jnp.concatenate([lo, hi], axis=0))
            srow = sall[e, 0] + sall[e, 1] + sall[e, 2] + sall[e, 3]
            eye = (lax.broadcasted_iota(jnp.int32, (BLK, BLK), 0) == lax.broadcasted_iota(jnp.int32, (BLK, BLK), 1))
            for i in range(nblk):
                col = jnp.sum(jnp.where(eye, srow[i:i + 1, :], 0.0), axis=1, keepdims=True)
                scol[i * BLK:(i + 1) * BLK, :] = jnp.broadcast_to(col, (BLK, BLK)) * two_h

        def project(e, t, value):
            ds = tile_ds(t)
            tb[:, ds] = value.astype(BF16)
            xb = (value - mu_ref[e, :, ds]).astype(BF16)
            part = jnp.dot(xb, u_ref[ds, :], preferred_element_type=F32)

            @pl.when(t == 0)
            def _():
                qacc[...] = part

            @pl.when(t > 0)
            def _():
                qacc[...] += part

        def update(e, t):
            ds = tile_ds(t)
            value = theta[e, :, ds]
            low = lax.dot_general(qall[e], u_ref[ds, :], TRANS_B, preferred_element_type=F32)
            centered = value - mu_ref[e, :, ds]
            grad = -(centered * lam_ref[:, ds] + low)
            mixed = (grad - two_h * value).astype(BF16)
            drive = jnp.dot(kfull[...], mixed, preferred_element_type=F32)
            new = value + gain * (drive + scol[:, 0:1] * value)
            theta[e, :, ds] = new
            return new

        def send_q(e):
            for i in range(nblk):
                pq[e, i] = qacc[i * BLK:(i + 1) * BLK, :]
            core_q(e).start()

        def gram(e):
            half = BLK // 2
            two = 2 * BLK

            def place(i, j, block):
                if i == j:
                    pg[e, i, 0:BLK, :] = block
                    eye = (lax.broadcasted_iota(jnp.int32, (BLK, BLK), 0) == lax.broadcasted_iota(jnp.int32, (BLK, BLK), 1))
                    pd[e, i:i + 1, :] = jnp.sum(jnp.where(eye, block, 0.0), axis=0, keepdims=True)
                elif j == i + 2:
                    pg[e, i, two:two + half, :] = block[0:half]
                    pg[e, i + 2, two:two + half, :] = block[half:BLK]
                else:
                    pg[e, 3 if (i, j) == (0, 3) else i, BLK:two, :] = block

            right = lax.dot_general(tb[...], tb[two:2 * two, :], TRANS_B, preferred_element_type=F32)
            for i in range(nblk):
                for j in (2, 3):
                    if i <= j:
                        place(i, j, right[i * BLK:(i + 1) * BLK, (j - 2) * BLK:(j - 1) * BLK])
            left = lax.dot_general(tb[0:two, :], tb[0:two, :], TRANS_B, preferred_element_type=F32)
            for i in range(2):
                for j in range(i, 2):
                    place(i, j, left[i * BLK:(i + 1) * BLK, j * BLK:(j + 1) * BLK])
            core_g(e).start()
            core_d(e).start()

        for e in range(2):
            for t in range(num_tiles):
                in_copy(e, t).start()
            pd[e] = jnp.zeros((8, BLK), F32)

        def first_pass(e, other):
            def body(t, carry):
                in_copy(e, t).wait()
                project(e, t, theta[e, :, tile_ds(t)])
                if other is not None:
                    services(other, t)
                return carry
            lax.fori_loop(0, num_tiles, body, 0)
            send_q(e)
            gram(e)

        def services(o, t):
            @pl.when(t == 0)
            def _():
                stage2_q(o)

            @pl.when(t == 2)
            def _():
                stage2_g(o)

            @pl.when(t == 4)
            def _():
                stage3_q(o)

        def finish(o):
            stage3_g(o)
            stage4(o, (0, 1, 2))
            stage5(o)

        first_pass(0, None)
        first_pass(1, 0)
        finish(0)

        def steady(i, carry):
            e = i % 2
            o = 1 - e

            def body(t, c):
                new = update(e, t)
                project(e, t, new)
                services(o, t)
                return c
            lax.fori_loop(0, num_tiles, body, 0)
            send_q(e)
            gram(e)
            finish(o)
            return carry

        lax.fori_loop(0, 2 * (NUM_STEPS - 1), steady, 0)

        def last0(t, c):
            update(0, t)
            out_copy(0, t).start()
            services(1, t)
            return c
        lax.fori_loop(0, num_tiles, last0, 0)
        finish(1)

        def last1(t, c):
            update(1, t)
            out_copy(1, t).start()
            return c
        lax.fori_loop(0, num_tiles, last1, 0)
        for e in range(2):
            for t in range(num_tiles):
                out_copy(e, t).wait()

    def call(particles, target_mean, precision, low_factor):
        vm = pl.BlockSpec(memory_space=pltpu.VMEM)
        hbm = pl.BlockSpec(memory_space=pl.ANY)
        scratch = [
            pltpu.VMEM((2, num_part, num_local), F32),
            pltpu.VMEM((num_part, num_local), BF16),
            pltpu.VMEM((num_part, num_part), BF16),
            pltpu.VMEM((num_part, BLK), F32),
            pltpu.VMEM((num_part, BLK), F32),
            pltpu.VMEM((2, nblk, BLK, BLK), F32),
            pltpu.VMEM((2, nblk, grow, BLK), F32),
            pltpu.VMEM((2, 8, BLK), F32),
            pltpu.VMEM((2, 2, BLK, BLK), F32),
            pltpu.VMEM((2, 2, grow, BLK), F32),
            pltpu.VMEM((2, 8, BLK), F32),
            pltpu.VMEM((2, 2, BLK, BLK), F32),
            pltpu.VMEM((2, 2, grow, BLK), F32),
            pltpu.VMEM((2, 8, BLK), F32),
            pltpu.VMEM((2, BLK, BLK), F32),
            pltpu.VMEM((2, grow, BLK), F32),
            pltpu.VMEM((2, 8, BLK), F32),
            pltpu.VMEM((8, BLK), F32),
            pltpu.VMEM((grow, BLK), F32),
            pltpu.VMEM((2, num_part, BLK), BF16),
            pltpu.VMEM((2, nblk, grow, BLK), BF16),
            pltpu.VMEM((2, nblk, 8, BLK), F32),
            pltpu.SemaphoreType.DMA((2, num_tiles)),
            pltpu.SemaphoreType.DMA((2, num_tiles)),
            pltpu.SemaphoreType.DMA((2, NUM_SEMS)),
            pltpu.SemaphoreType.DMA((2, NUM_SEMS)),
        ]
        return pl.pallas_call(
            kernel,
            out_shape=jax.ShapeDtypeStruct(particles.shape, F32),
            in_specs=[hbm, vm, vm, vm],
            out_specs=hbm,
            scratch_shapes=scratch,
            compiler_params=pltpu.CompilerParams(
                collective_id=0, has_side_effects=True, vmem_limit_bytes=60 * 1024 * 1024),
            cost_estimate=pl.CostEstimate(flops=33 * 10**9, bytes_accessed=36 * 2**20, transcendentals=0),
        )(particles, target_mean[:, None, :], precision[None, :], low_factor)

    return call


def solution(mesh):
    feat_count = mesh.shape["feat"]
    data_spec = P("ens", None, "feat")

    def local_steps(particles, target_mean, precision, low_factor):
        num_part, num_local = particles.shape[1], particles.shape[2]
        call = build_kernel(num_part, num_local, num_local * feat_count)
        return call(particles, target_mean, precision, low_factor)

    return jax.shard_map(
        local_steps, mesh=mesh,
        in_specs=(data_spec, P("ens", "feat"), P(("ens", "feat")), P(("ens", "feat"), None)),
        out_specs=data_spec, check_vma=False)
```

```python
import jax
import jax.numpy as jnp
from jax import lax
from jax.experimental import pallas as pl
from jax.experimental.pallas import tpu as pltpu
from jax.sharding import PartitionSpec as P

NUM_STEPS = 3
OUT_HBM = True
POS = 0
MIX_T = 5
DRV_T = 1
BLK = 128
TILE = 512
F32 = jnp.float32
BF16 = jnp.bfloat16
TRANS_B = (((1,), (1,)), ((), ()))

SEM_CORE, SEM_CHIP, SEM_GATHER, SEM_OWN, SEM_FWD = range(5)
NUM_KINDS = 3
NUM_SEMS = 5 * NUM_KINDS


def build_kernel(num_part, num_local, total_feat):
    nblk = num_part // BLK
    num_tiles = num_local // TILE
    bandwidth = 2.0 * total_feat
    step_size = 0.25 * total_feat
    two_h = 2.0 / bandwidth
    gain = step_size / num_part
    grow = 2 * BLK + BLK // 2

    def kernel(th_hbm, mu_ref, lam_ref, u_ref, out_hbm,
               theta, tb, xb, ybuf, kfull, scol,
               pq, pg, pd, rq, rg, rd, sq, sg, sd, xq, xg, xd, dfull, gsum,
               qall, kall, sall,
               in_sem, out_sem, send_sem, recv_sem):
        feat = lax.axis_index("feat")
        chip = feat // 2
        core = feat % 2
        own = 2 * core + chip
        peer_core = {"feat": 2 * chip + (1 - core)}
        peer_chip = {"feat": 2 * (1 - chip) + core}

        def rcopy(src, dst, e, group, kind, peer):
            idx = group * NUM_KINDS + kind
            return pltpu.make_async_remote_copy(
                src_ref=src, dst_ref=dst, send_sem=send_sem.at[e, idx], recv_sem=recv_sem.at[e, idx],
                device_id=peer, device_id_type=pl.DeviceIdType.MESH)

        def tile_ds(t):
            return pl.ds(pl.multiple_of(t * TILE, TILE), TILE)

        def in_copy(e, t):
            return pltpu.make_async_copy(th_hbm.at[e, :, tile_ds(t)], theta.at[e, :, tile_ds(t)], in_sem.at[e, t])

        def out_copy(e, t):
            return pltpu.make_async_copy(theta.at[e, :, tile_ds(t)], out_hbm.at[e, :, tile_ds(t)], out_sem.at[e, t])

        def core_q(e):
            return rcopy(pq.at[e, pl.ds(2 * (1 - core), 2)], rq.at[e], e, SEM_CORE, 0, peer_core)

        def core_g(e):
            return rcopy(pg.at[e, pl.ds(2 * (1 - core), 2)], rg.at[e], e, SEM_CORE, 1, peer_core)

        def core_d(e):
            return rcopy(pd.at[e], rd.at[e], e, SEM_CORE, 2, peer_core)

        def chip_q(e):
            return rcopy(sq.at[e, 1 - chip], xq.at[e], e, SEM_CHIP, 0, peer_chip)

        def chip_g(e):
            return rcopy(sg.at[e, 1 - chip], xg.at[e], e, SEM_CHIP, 1, peer_chip)

        def chip_d(e):
            return rcopy(sd.at[e], xd.at[e], e, SEM_CHIP, 2, peer_chip)

        def gather(e, slot, group, kind, peer):
            buf = (qall, kall, sall)[kind]
            if kind == 0:
                ref = buf.at[e, pl.ds(pl.multiple_of(slot * BLK, BLK), BLK)]
            else:
                ref = buf.at[e, slot]
            return rcopy(ref, ref, e, group, kind, peer)

        def to_chip(e, kind):
            return gather(e, own, SEM_GATHER, kind, peer_chip)

        def to_core(e, kind):
            return gather(e, own, SEM_OWN, kind, peer_core)

        def forward(e, kind):
            return gather(e, 2 * core + (1 - chip), SEM_FWD, kind, peer_core)

        def stage2_q(e):
            core_q(e).wait()
            for c in range(2):
                sq[e, c] = pq[e, 2 * core + c] + rq[e, c]
            chip_q(e).start()

        def stage2_g(e):
            core_g(e).wait()
            core_d(e).wait()
            sd[e] = pd[e] + rd[e]
            chip_d(e).start()
            for c in range(2):
                sg[e, c] = pg[e, 2 * core + c] + rg[e, c]
            chip_g(e).start()

        def stage3_q(e):
            chip_q(e).wait()
            full = sq[e, chip] + xq[e]
            qall[e, pl.ds(pl.multiple_of(own * BLK, BLK), BLK), :] = full.astype(BF16)
            to_chip(e, 0).start()
            to_core(e, 0).start()

        def stage3_g(e):
            chip_d(e).wait()
            chip_g(e).wait()
            dfull[...] = sd[e] + xd[e]
            gsum[...] = sg[e, chip] + xg[e]
            sall[e, own] = jnp.zeros((8, BLK), F32)
            wrap = own // 3
            half = own // 2
            parts = (
                (0, BLK, own, own, 0),
                (BLK, BLK, own - 3 * wrap, own + 1 - wrap, 0),
                (2 * BLK, BLK // 2, own % 2, own % 2 + 2, half * (BLK // 2)),
            )
            for index, (start, size, row_blk, col_blk, row_off) in enumerate(parts):
                row_id = lax.broadcasted_iota(jnp.int32, (size, BLK), 0) + row_off
                col_id = lax.broadcasted_iota(jnp.int32, (size, BLK), 1)
                eye = row_id == col_id
                diag_col = jnp.sum(jnp.where(eye, dfull[pl.ds(row_blk, 1), :], 0.0), axis=1, keepdims=True)
                diag_row = dfull[pl.ds(col_blk, 1), :]
                dist = jnp.maximum(diag_col + diag_row - 2.0 * gsum[start:start + size, :], 0.0)
                kern = jnp.exp(-dist / bandwidth)
                kall[e, own, start:start + size, :] = kern.astype(BF16)
                sall[e, own, pl.ds(col_blk, 1), :] += jnp.sum(kern, axis=0, keepdims=True)
                if index > 0:
                    row_sum = jnp.sum(kern, axis=1, keepdims=True)
                    sall[e, own, pl.ds(row_blk, 1), :] += jnp.sum(jnp.where(eye, row_sum, 0.0), axis=0, keepdims=True)
            for kind in (1, 2):
                to_chip(e, kind).start()
                to_core(e, kind).start()

        def stage4(e, kinds):
            for kind in kinds:
                to_chip(e, kind).wait()
                forward(e, kind).start()

        def stage5_q(e):
            to_core(e, 0).wait()
            forward(e, 0).wait()

        def stage5(e):
            for kind in (1, 2):
                to_core(e, kind).wait()
                forward(e, kind).wait()
            half = BLK // 2

            def put(i, j, rows, block):
                r0 = i * BLK + rows
                n = block.shape[0]
                kfull[r0:r0 + n, j * BLK:(j + 1) * BLK] = (block * gain).astype(BF16)

            def put_pair(i, j, block):
                put(i, j, 0, block)
                put(j, i, 0, block.T)

            for i in range(nblk):
                put(i, i, 0, kall[e, i, 0:BLK, :].astype(F32))
            for i, j, o in ((0, 1, 0), (1, 2, 1), (2, 3, 2), (0, 3, 3)):
                put_pair(i, j, kall[e, o, BLK:2 * BLK, :].astype(F32))
            for i in range(2):
                lo = kall[e, i, 2 * BLK:2 * BLK + half, :]
                hi = kall[e, i + 2, 2 * BLK:2 * BLK + half, :]
                put_pair(i, i + 2, jnp.concatenate([lo, hi], axis=0).astype(F32))
            srow = sall[e, 0] + sall[e, 1] + sall[e, 2] + sall[e, 3]
            eye = (lax.broadcasted_iota(jnp.int32, (BLK, BLK), 0) == lax.broadcasted_iota(jnp.int32, (BLK, BLK), 1))
            for i in range(nblk):
                col = jnp.sum(jnp.where(eye, srow[i:i + 1, :], 0.0), axis=1, keepdims=True)
                scol[i * BLK:(i + 1) * BLK, :] = 1.0 + jnp.broadcast_to(col, (BLK, BLK)) * (gain * two_h)

        def round_inputs(e, t, value):
            ds = tile_ds(t)
            tb[:, ds] = value.astype(BF16)
            xb[:, ds] = (value - mu_ref[pl.ds(e, 1), ds]).astype(BF16)

        def mix(e, t):
            ds = tile_ds(t)
            value = theta[e, :, ds]
            low = lax.dot_general(qall[e], u_ref[ds, :], TRANS_B, preferred_element_type=F32)
            centered = value - mu_ref[pl.ds(e, 1), ds]
            ybuf[:, ds] = (centered * (lam_ref[:, ds] + two_h) + (low + two_h * mu_ref[pl.ds(e, 1), ds])).astype(BF16)

        def drive(e, t):
            ds = tile_ds(t)
            moved = jnp.dot(kfull[...], ybuf[:, ds], preferred_element_type=F32)
            new = theta[e, :, ds] * scol[:, 0:1] - moved
            theta[e, :, ds] = new
            return new

        def send_q(e):
            hk = num_local // 2

            @pl.when(feat >= 0)
            def _():
                part = [jnp.dot(xb[:, k * hk:(k + 1) * hk], u_ref[k * hk:(k + 1) * hk, :], preferred_element_type=F32) for k in range(2)]
                part = part[0] + part[1]
                for i in range(nblk):
                    pq[e, i] = part[i * BLK:(i + 1) * BLK, :]
            core_q(e).start()

        def gram(e, o):
            half = BLK // 2
            two = 2 * BLK

            def place(i, j, block):
                if i == j:
                    pg[e, i, 0:BLK, :] = block
                    eye = (lax.broadcasted_iota(jnp.int32, (BLK, BLK), 0) == lax.broadcasted_iota(jnp.int32, (BLK, BLK), 1))
                    pd[e, i:i + 1, :] = jnp.sum(jnp.where(eye, block, 0.0), axis=0, keepdims=True)
                elif j == i + 2:
                    pg[e, i, two:two + half, :] = block[0:half]
                    pg[e, i + 2, two:two + half, :] = block[half:BLK]
                else:
                    pg[e, 3 if (i, j) == (0, 3) else i, BLK:two, :] = block

            @pl.when(feat >= 0)
            def _():
                right = lax.dot_general(tb[...], tb[two:2 * two, :], TRANS_B, preferred_element_type=F32)
                left = lax.dot_general(tb[0:two, :], tb[0:two, :], TRANS_B, preferred_element_type=F32)
                for i in range(nblk):
                    for j in (2, 3):
                        if i <= j:
                            place(i, j, right[i * BLK:(i + 1) * BLK, (j - 2) * BLK:(j - 1) * BLK])
                for i in range(2):
                    for j in range(i, 2):
                        place(i, j, left[i * BLK:(i + 1) * BLK, j * BLK:(j + 1) * BLK])
            core_g(e).start()
            core_d(e).start()
            stage2_q(e)

        for e in range(2):
            pd[e] = jnp.zeros((8, BLK), F32)

        def loop(num, body):
            lax.fori_loop(0, num, lambda t, c: (body(t), c)[1], 0)

        def at(t, when, fn, *args):
            @pl.when(t == when)
            def _():
                fn(*args)

        def first_pass(e):
            def body(t):
                in_copy(e, t).wait()
                round_inputs(e, t, theta[e, :, tile_ds(t)])
            loop(num_tiles, body)

        for e in range(2):
            for t in range(num_tiles):
                in_copy(e, t).start()
        barrier = pltpu.get_barrier_semaphore()
        for peer in (peer_core, peer_chip):
            pl.semaphore_signal(barrier, inc=1, device_id=peer, device_id_type=pl.DeviceIdType.MESH)
        first_pass(0)
        pl.semaphore_wait(barrier, 2)
        send_q(0)
        gram(0, None)
        first_pass(1)
        stage2_g(0)
        send_q(1)
        stage3_q(0)
        gram(1, 0)
        if POS == 0:
            stage3_g(0)
        stage4(0, (0,))

        def half_step(e, last, others):
            o = 1 - e
            stage5_q(e)

            def mix_body(t):
                mix(e, t)
                if others:
                    at(t, MIX_T, stage2_g, o)
            loop(num_tiles, mix_body)
            stage4(e, (1, 2))
            stage5(e)

            def drive_body(t):
                new = drive(e, t)
                if last:
                    if OUT_HBM:
                        out_copy(e, t).start()
                else:
                    round_inputs(e, t, new)
                if others:
                    at(t, DRV_T, stage3_q, o)
            loop(num_tiles, drive_body)
            if not last:
                send_q(e)
            if others:
                stage4(o, (0,))
            if POS == 0 and others:
                stage3_g(o)
            if not last:
                gram(e, o)
            elif POS == 1 and others:
                stage3_g(o)

        def steady(i, carry):
            half_step(i % 2, False, True)
            return carry

        lax.fori_loop(0, 2 * (NUM_STEPS - 1), steady, 0)
        half_step(0, True, True)
        half_step(1, True, False)
        if OUT_HBM:
            for e in range(2):
                for t in range(num_tiles):
                    out_copy(e, t).wait()

    def call(particles, target_mean, precision, low_factor):
        vm = pl.BlockSpec(memory_space=pltpu.VMEM)
        hbm = pl.BlockSpec(memory_space=pl.ANY)
        scratch = [
            pltpu.VMEM((2, num_part, num_local), F32),
            pltpu.VMEM((num_part, num_local), BF16),
            pltpu.VMEM((num_part, num_local), BF16),
            pltpu.VMEM((num_part, num_local), BF16),
            pltpu.VMEM((num_part, num_part), BF16),
            pltpu.VMEM((num_part, BLK), F32),
            pltpu.VMEM((2, nblk, BLK, BLK), F32),
            pltpu.VMEM((2, nblk, grow, BLK), F32),
            pltpu.VMEM((2, 8, BLK), F32),
            pltpu.VMEM((2, 2, BLK, BLK), F32),
            pltpu.VMEM((2, 2, grow, BLK), F32),
            pltpu.VMEM((2, 8, BLK), F32),
            pltpu.VMEM((2, 2, BLK, BLK), F32),
            pltpu.VMEM((2, 2, grow, BLK), F32),
            pltpu.VMEM((2, 8, BLK), F32),
            pltpu.VMEM((2, BLK, BLK), F32),
            pltpu.VMEM((2, grow, BLK), F32),
            pltpu.VMEM((2, 8, BLK), F32),
            pltpu.VMEM((8, BLK), F32),
            pltpu.VMEM((grow, BLK), F32),
            pltpu.VMEM((2, num_part, BLK), BF16),
            pltpu.VMEM((2, nblk, grow, BLK), BF16),
            pltpu.VMEM((2, nblk, 8, BLK), F32),
            pltpu.SemaphoreType.DMA((2, num_tiles)),
            pltpu.SemaphoreType.DMA((2, num_tiles)),
            pltpu.SemaphoreType.DMA((2, NUM_SEMS)),
            pltpu.SemaphoreType.DMA((2, NUM_SEMS)),
        ]
        return pl.pallas_call(
            kernel,
            out_shape=jax.ShapeDtypeStruct(particles.shape, F32),
            in_specs=[hbm, vm, vm, vm],
            out_specs=hbm,
            scratch_shapes=scratch,
            compiler_params=pltpu.CompilerParams(
                collective_id=0, has_side_effects=True, vmem_limit_bytes=60 * 1024 * 1024),
            cost_estimate=pl.CostEstimate(flops=33 * 10**9, bytes_accessed=36 * 2**20, transcendentals=0),
        )(particles, target_mean, precision[None, :], low_factor)

    return call


def solution(mesh):
    feat_count = mesh.shape["feat"]
    data_spec = P("ens", None, "feat")

    def local_steps(particles, target_mean, precision, low_factor):
        num_part, num_local = particles.shape[1], particles.shape[2]
        call = build_kernel(num_part, num_local, num_local * feat_count)
        return call(particles, target_mean, precision, low_factor)

    return jax.shard_map(
        local_steps, mesh=mesh,
        in_specs=(data_spec, P("ens", "feat"), P(("ens", "feat")), P(("ens", "feat"), None)),
        out_specs=data_spec, check_vma=False)
```

```python
import jax
import jax.numpy as jnp
from jax import lax
from jax.experimental import pallas as pl
from jax.experimental.pallas import tpu as pltpu
from jax.sharding import PartitionSpec as P

NUM_STEPS = 3
MIX_T = 5
DRV_T = 1
BLK = 128
TILE = 512
F32 = jnp.float32
BF16 = jnp.bfloat16
TRANS_B = (((1,), (1,)), ((), ()))

SEM_CORE, SEM_CHIP, SEM_GATHER, SEM_OWN, SEM_FWD = range(5)
NUM_KINDS = 3
NUM_SEMS = 5 * NUM_KINDS


def build_kernel(num_part, num_local, total_feat):
    nblk = num_part // BLK
    num_tiles = num_local // TILE
    bandwidth = 2.0 * total_feat
    step_size = 0.25 * total_feat
    two_h = 2.0 / bandwidth
    gain = step_size / num_part
    grow = 2 * BLK + BLK // 2

    def kernel(th_hbm, mu_ref, lam_ref, u_ref, theta, ybuf, kfull, scol,
               tb, xb,
               pq, pg, pd, rq, rg, rd, sq, sg, sd, xq, xg, xd, dfull, gsum,
               qall, kall, sall,
               in_sem, send_sem, recv_sem):
        feat = lax.axis_index("feat")
        chip = feat // 2
        core = feat % 2
        own = 2 * core + chip
        peer_core = {"feat": 2 * chip + (1 - core)}
        peer_chip = {"feat": 2 * (1 - chip) + core}

        def rcopy(src, dst, e, group, kind, peer):
            idx = group * NUM_KINDS + kind
            return pltpu.make_async_remote_copy(
                src_ref=src, dst_ref=dst, send_sem=send_sem.at[e, idx], recv_sem=recv_sem.at[e, idx],
                device_id=peer, device_id_type=pl.DeviceIdType.MESH)

        def tile_ds(t):
            return pl.ds(pl.multiple_of(t * TILE, TILE), TILE)

        def in_copy(e, t):
            return pltpu.make_async_copy(th_hbm.at[e, :, tile_ds(t)], theta.at[e, :, tile_ds(t)], in_sem.at[e, t])

        def core_q(e):
            return rcopy(pq.at[e, pl.ds(2 * (1 - core), 2)], rq.at[e], e, SEM_CORE, 0, peer_core)

        def core_g(e):
            return rcopy(pg.at[e, pl.ds(2 * (1 - core), 2)], rg.at[e], e, SEM_CORE, 1, peer_core)

        def core_d(e):
            return rcopy(pd.at[e], rd.at[e], e, SEM_CORE, 2, peer_core)

        def chip_q(e):
            return rcopy(sq.at[e, 1 - chip], xq.at[e], e, SEM_CHIP, 0, peer_chip)

        def chip_g(e):
            return rcopy(sg.at[e, 1 - chip], xg.at[e], e, SEM_CHIP, 1, peer_chip)

        def chip_d(e):
            return rcopy(sd.at[e], xd.at[e], e, SEM_CHIP, 2, peer_chip)

        def gather(e, slot, group, kind, peer):
            buf = (qall, kall, sall)[kind]
            if kind == 0:
                ref = buf.at[e, pl.ds(pl.multiple_of(slot * BLK, BLK), BLK)]
            else:
                ref = buf.at[e, slot]
            return rcopy(ref, ref, e, group, kind, peer)

        def to_chip(e, kind):
            return gather(e, own, SEM_GATHER, kind, peer_chip)

        def to_core(e, kind):
            return gather(e, own, SEM_OWN, kind, peer_core)

        def forward(e, kind):
            return gather(e, 2 * core + (1 - chip), SEM_FWD, kind, peer_core)

        def stage2_q(e):
            core_q(e).wait()
            for c in range(2):
                sq[e, c] = pq[e, 2 * core + c] + rq[e, c]
            chip_q(e).start()

        def stage2_g(e):
            core_g(e).wait()
            core_d(e).wait()
            sd[e] = pd[e] + rd[e]
            chip_d(e).start()
            for c in range(2):
                sg[e, c] = pg[e, 2 * core + c] + rg[e, c]
            chip_g(e).start()

        def stage3_q(e):
            chip_q(e).wait()
            full = sq[e, chip] + xq[e]
            qall[e, pl.ds(pl.multiple_of(own * BLK, BLK), BLK), :] = full.astype(BF16)
            to_chip(e, 0).start()
            to_core(e, 0).start()

        def stage3_g(e):
            chip_d(e).wait()
            chip_g(e).wait()
            dfull[...] = sd[e] + xd[e]
            gsum[...] = sg[e, chip] + xg[e]
            sall[e, own] = jnp.zeros((8, BLK), F32)
            wrap = own // 3
            half = own // 2
            parts = (
                (0, BLK, own, own, 0),
                (BLK, BLK, own - 3 * wrap, own + 1 - wrap, 0),
                (2 * BLK, BLK // 2, own % 2, own % 2 + 2, half * (BLK // 2)),
            )
            for index, (start, size, row_blk, col_blk, row_off) in enumerate(parts):
                row_id = lax.broadcasted_iota(jnp.int32, (size, BLK), 0) + row_off
                col_id = lax.broadcasted_iota(jnp.int32, (size, BLK), 1)
                eye = row_id == col_id
                diag_col = jnp.sum(jnp.where(eye, dfull[pl.ds(row_blk, 1), :], 0.0), axis=1, keepdims=True)
                diag_row = dfull[pl.ds(col_blk, 1), :]
                dist = jnp.maximum(diag_col + diag_row - 2.0 * gsum[start:start + size, :], 0.0)
                kern = jnp.exp(-dist / bandwidth)
                kall[e, own, start:start + size, :] = kern.astype(BF16)
                sall[e, own, pl.ds(col_blk, 1), :] += jnp.sum(kern, axis=0, keepdims=True)
                if index > 0:
                    row_sum = jnp.sum(kern, axis=1, keepdims=True)
                    sall[e, own, pl.ds(row_blk, 1), :] += jnp.sum(jnp.where(eye, row_sum, 0.0), axis=0, keepdims=True)
            for kind in (1, 2):
                to_chip(e, kind).start()
                to_core(e, kind).start()

        def stage4(e, kinds):
            for kind in kinds:
                to_chip(e, kind).wait()
                forward(e, kind).start()

        def stage5_q(e):
            to_core(e, 0).wait()
            forward(e, 0).wait()

        def stage5(e):
            for kind in (1, 2):
                to_core(e, kind).wait()
                forward(e, kind).wait()
            half = BLK // 2

            def put(i, j, rows, block):
                r0 = i * BLK + rows
                n = block.shape[0]
                kfull[r0:r0 + n, j * BLK:(j + 1) * BLK] = (block * gain).astype(BF16)

            def put_pair(i, j, block):
                put(i, j, 0, block)
                put(j, i, 0, block.T)

            for i in range(nblk):
                put(i, i, 0, kall[e, i, 0:BLK, :].astype(F32))
            for i, j, o in ((0, 1, 0), (1, 2, 1), (2, 3, 2), (0, 3, 3)):
                put_pair(i, j, kall[e, o, BLK:2 * BLK, :].astype(F32))
            for i in range(2):
                lo = kall[e, i, 2 * BLK:2 * BLK + half, :]
                hi = kall[e, i + 2, 2 * BLK:2 * BLK + half, :]
                put_pair(i, i + 2, jnp.concatenate([lo, hi], axis=0).astype(F32))
            srow = sall[e, 0] + sall[e, 1] + sall[e, 2] + sall[e, 3]
            eye = (lax.broadcasted_iota(jnp.int32, (BLK, BLK), 0) == lax.broadcasted_iota(jnp.int32, (BLK, BLK), 1))
            for i in range(nblk):
                col = jnp.sum(jnp.where(eye, srow[i:i + 1, :], 0.0), axis=1, keepdims=True)
                scol[i * BLK:(i + 1) * BLK, :] = 1.0 + jnp.broadcast_to(col, (BLK, BLK)) * (gain * two_h)

        def round_inputs(e, t, value):
            ds = tile_ds(t)
            tb[:, ds] = value.astype(BF16)
            xb[:, ds] = (value - mu_ref[pl.ds(e, 1), ds]).astype(BF16)

        def mix(e, t):
            ds = tile_ds(t)
            value = theta[e, :, ds]
            low = lax.dot_general(qall[e], u_ref[ds, :], TRANS_B, preferred_element_type=F32)
            centered = value - mu_ref[pl.ds(e, 1), ds]
            ybuf[:, ds] = (centered * (lam_ref[:, ds] + two_h) + (low + two_h * mu_ref[pl.ds(e, 1), ds])).astype(BF16)

        def drive(e, t):
            ds = tile_ds(t)
            moved = jnp.dot(kfull[...], ybuf[:, ds], preferred_element_type=F32)
            new = theta[e, :, ds] * scol[:, 0:1] - moved
            theta[e, :, ds] = new
            return new

        def send_q(e):
            hk = num_local // 2

            @pl.when(feat >= 0)
            def _():
                part = [jnp.dot(xb[:, k * hk:(k + 1) * hk], u_ref[k * hk:(k + 1) * hk, :], preferred_element_type=F32) for k in range(2)]
                part = part[0] + part[1]
                for i in range(nblk):
                    pq[e, i] = part[i * BLK:(i + 1) * BLK, :]
            core_q(e).start()

        def gram(e):
            half = BLK // 2
            two = 2 * BLK

            def place(i, j, block):
                if i == j:
                    pg[e, i, 0:BLK, :] = block
                    eye = (lax.broadcasted_iota(jnp.int32, (BLK, BLK), 0) == lax.broadcasted_iota(jnp.int32, (BLK, BLK), 1))
                    pd[e, i:i + 1, :] = jnp.sum(jnp.where(eye, block, 0.0), axis=0, keepdims=True)
                elif j == i + 2:
                    pg[e, i, two:two + half, :] = block[0:half]
                    pg[e, i + 2, two:two + half, :] = block[half:BLK]
                else:
                    pg[e, 3 if (i, j) == (0, 3) else i, BLK:two, :] = block

            @pl.when(feat >= 0)
            def _():
                right = lax.dot_general(tb[...], tb[two:2 * two, :], TRANS_B, preferred_element_type=F32)
                left = lax.dot_general(tb[0:two, :], tb[0:two, :], TRANS_B, preferred_element_type=F32)
                for i in range(nblk):
                    for j in (2, 3):
                        if i <= j:
                            place(i, j, right[i * BLK:(i + 1) * BLK, (j - 2) * BLK:(j - 1) * BLK])
                for i in range(2):
                    for j in range(i, 2):
                        place(i, j, left[i * BLK:(i + 1) * BLK, j * BLK:(j + 1) * BLK])
            core_g(e).start()
            core_d(e).start()
            stage2_q(e)

        for e in range(2):
            pd[e] = jnp.zeros((8, BLK), F32)

        def loop(num, body):
            lax.fori_loop(0, num, lambda t, c: (body(t), c)[1], 0)

        def at(t, when, fn, *args):
            @pl.when(t == when)
            def _():
                fn(*args)

        def first_pass(e):
            def body(t):
                in_copy(e, t).wait()
                round_inputs(e, t, theta[e, :, tile_ds(t)])
            loop(num_tiles, body)

        for e in range(2):
            for t in range(num_tiles):
                in_copy(e, t).start()
        barrier = pltpu.get_barrier_semaphore()
        for peer in (peer_core, peer_chip):
            pl.semaphore_signal(barrier, inc=1, device_id=peer, device_id_type=pl.DeviceIdType.MESH)
        first_pass(0)
        pl.semaphore_wait(barrier, 2)
        send_q(0)
        gram(0)
        first_pass(1)
        stage2_g(0)
        send_q(1)
        stage3_q(0)
        gram(1)
        stage3_g(0)
        stage4(0, (0,))

        def finish_mix(e, o):
            stage5_q(e)

            def mix_body(t):
                mix(e, t)
                if o is not None:
                    at(t, MIX_T, stage2_g, o)
            loop(num_tiles, mix_body)
            stage4(e, (1, 2))
            stage5(e)

        def half_step(e, last):
            o = 1 - e
            finish_mix(e, o)

            def drive_body(t):
                new = drive(e, t)
                if not last:
                    round_inputs(e, t, new)
                at(t, DRV_T, stage3_q, o)
            loop(num_tiles, drive_body)
            if not last:
                send_q(e)
            stage4(o, (0,))
            stage3_g(o)
            if not last:
                gram(e)

        def steady(i, carry):
            half_step(i % 2, False)
            return carry

        lax.fori_loop(0, 2 * (NUM_STEPS - 1), steady, 0)
        half_step(0, True)
        finish_mix(1, None)

    def last_kernel(theta, ybuf, kfull, scol, out_hbm, new, out_sem):
        first = pltpu.make_async_copy(theta.at[0], out_hbm.at[0], out_sem.at[num_tiles])
        first.start()

        def out_copy(t):
            ds = pl.ds(pl.multiple_of(t * TILE, TILE), TILE)
            return pltpu.make_async_copy(new.at[:, ds], out_hbm.at[1, :, ds], out_sem.at[t])

        def body(t, carry):
            ds = pl.ds(pl.multiple_of(t * TILE, TILE), TILE)
            moved = jnp.dot(kfull[...], ybuf[:, ds], preferred_element_type=F32)
            new[:, ds] = theta[1, :, ds] * scol[:, 0:1] - moved
            out_copy(t).start()
            return carry

        lax.fori_loop(0, num_tiles, body, 0)
        first.wait()
        for t in range(num_tiles):
            out_copy(t).wait()

    def call(particles, target_mean, precision, low_factor):
        vm = pl.BlockSpec(memory_space=pltpu.VMEM)
        hbm = pl.BlockSpec(memory_space=pl.ANY)
        scratch = [
            pltpu.VMEM((num_part, num_local), BF16),
            pltpu.VMEM((num_part, num_local), BF16),
            pltpu.VMEM((2, nblk, BLK, BLK), F32),
            pltpu.VMEM((2, nblk, grow, BLK), F32),
            pltpu.VMEM((2, 8, BLK), F32),
            pltpu.VMEM((2, 2, BLK, BLK), F32),
            pltpu.VMEM((2, 2, grow, BLK), F32),
            pltpu.VMEM((2, 8, BLK), F32),
            pltpu.VMEM((2, 2, BLK, BLK), F32),
            pltpu.VMEM((2, 2, grow, BLK), F32),
            pltpu.VMEM((2, 8, BLK), F32),
            pltpu.VMEM((2, BLK, BLK), F32),
            pltpu.VMEM((2, grow, BLK), F32),
            pltpu.VMEM((2, 8, BLK), F32),
            pltpu.VMEM((8, BLK), F32),
            pltpu.VMEM((grow, BLK), F32),
            pltpu.VMEM((2, num_part, BLK), BF16),
            pltpu.VMEM((2, nblk, grow, BLK), BF16),
            pltpu.VMEM((2, nblk, 8, BLK), F32),
            pltpu.SemaphoreType.DMA((2, num_tiles)),
            pltpu.SemaphoreType.DMA((2, NUM_SEMS)),
            pltpu.SemaphoreType.DMA((2, NUM_SEMS)),
        ]
        state = pl.pallas_call(
            kernel,
            out_shape=(pltpu.VMEM(particles.shape, F32), pltpu.VMEM((num_part, num_local), BF16),
                       pltpu.VMEM((num_part, num_part), BF16), pltpu.VMEM((num_part, BLK), F32)),
            in_specs=[hbm, vm, vm, vm],
            out_specs=(vm, vm, vm, vm),
            scratch_shapes=scratch,
            compiler_params=pltpu.CompilerParams(
                collective_id=0, has_side_effects=True, vmem_limit_bytes=36 * 1024 * 1024),
            cost_estimate=pl.CostEstimate(flops=30 * 10**9, bytes_accessed=18 * 2**20, transcendentals=0),
        )(particles, target_mean, precision[None, :], low_factor)
        return pl.pallas_call(
            last_kernel,
            out_shape=jax.ShapeDtypeStruct(particles.shape, F32),
            in_specs=[vm, vm, vm, vm],
            out_specs=hbm,
            scratch_shapes=[pltpu.VMEM((num_part, num_local), F32), pltpu.SemaphoreType.DMA((num_tiles + 1,))],
            compiler_params=pltpu.CompilerParams(vmem_limit_bytes=10 * 1024 * 1024),
            cost_estimate=pl.CostEstimate(flops=2 * 10**9, bytes_accessed=16 * 2**20, transcendentals=0),
        )(*state)

    return call


def solution(mesh):
    feat_count = mesh.shape["feat"]
    data_spec = P("ens", None, "feat")

    def local_steps(particles, target_mean, precision, low_factor):
        num_part, num_local = particles.shape[1], particles.shape[2]
        call = build_kernel(num_part, num_local, num_local * feat_count)
        return call(particles, target_mean, precision, low_factor)

    return jax.shard_map(
        local_steps, mesh=mesh,
        in_specs=(data_spec, P("ens", "feat"), P(("ens", "feat")), P(("ens", "feat"), None)),
        out_specs=data_spec, check_vma=False)
```

```python
import jax
import jax.numpy as jnp
from jax import lax
from jax.experimental import pallas as pl
from jax.experimental.pallas import tpu as pltpu
from jax.sharding import PartitionSpec as P

NUM_STEPS = 3
BLK = 128
TILE = 512
MTILE = 1024
DTILE = 2048
T2D = 1
T4O = 1
T2O = 2
S3 = 0
F32 = jnp.float32
BF16 = jnp.bfloat16
TRANS_B = (((1,), (1,)), ((), ()))

SEM_CORE, SEM_CHIP, SEM_GATHER, SEM_OWN, SEM_FWD = range(5)
KIND_Q, KIND_DIAG, KIND_OFF, KIND_VEC = range(4)
NUM_KINDS = 4
NUM_SEMS = 5 * NUM_KINDS


def build_kernel(num_part, num_local, total_feat):
    nblk = num_part // BLK
    num_tiles = num_local // TILE
    bandwidth = 2.0 * total_feat
    step_size = 0.25 * total_feat
    two_h = 2.0 / bandwidth
    gain = step_size / num_part
    piece = BLK // nblk
    diag_blocks = ((0, 0), (0, 1), (1, 1), (2, 2), (2, 3), (3, 3))
    off_blocks = ((0, 2), (0, 3), (1, 2), (1, 3))
    blocks = diag_blocks + off_blocks
    grow = piece * len(blocks)
    split = piece * len(diag_blocks)
    spans = {KIND_DIAG: pl.ds(0, split), KIND_OFF: pl.ds(split, grow - split)}

    def kernel(th_hbm, mu_ref, lam_ref, u_ref, theta, ybuf, kfull, scol,
               tb, xb,
               pq, pg, pd, rq, rg, rd, sq, sg, sd, xq, xg, xd, dfull,
               qall, kall, sall,
               in_sem, send_sem, recv_sem):
        feat = lax.axis_index("feat")
        chip = feat // 2
        core = feat % 2
        own = 2 * core + chip
        peer_core = {"feat": 2 * chip + (1 - core)}
        peer_chip = {"feat": 2 * (1 - chip) + core}

        def rcopy(src, dst, e, group, kind, peer):
            idx = group * NUM_KINDS + kind
            return pltpu.make_async_remote_copy(
                src_ref=src, dst_ref=dst, send_sem=send_sem.at[e, idx], recv_sem=recv_sem.at[e, idx],
                device_id=peer, device_id_type=pl.DeviceIdType.MESH)

        def tile_ds(t, size=TILE):
            return pl.ds(pl.multiple_of(t * size, size), size)

        def in_copy(e, t):
            return pltpu.make_async_copy(th_hbm.at[e, :, tile_ds(t)], theta.at[e, :, tile_ds(t)], in_sem.at[e, t])

        def core_reduce(e, kind):
            if kind == KIND_Q:
                src, dst = pq.at[e, pl.ds(2 * (1 - core), 2)], rq.at[e]
            elif kind == KIND_VEC:
                src, dst = pd.at[e], rd.at[e]
            else:
                src, dst = pg.at[e, pl.ds(2 * (1 - core), 2), spans[kind]], rg.at[e, :, spans[kind]]
            return rcopy(src, dst, e, SEM_CORE, kind, peer_core)

        def chip_reduce(e, kind):
            if kind == KIND_Q:
                src, dst = sq.at[e, 1 - chip], xq.at[e]
            elif kind == KIND_VEC:
                src, dst = sd.at[e], xd.at[e]
            else:
                src, dst = sg.at[e, 1 - chip, spans[kind]], xg.at[e, spans[kind]]
            return rcopy(src, dst, e, SEM_CHIP, kind, peer_chip)

        def gather(e, slot, group, kind, peer):
            if kind == KIND_Q:
                ref = qall.at[e, pl.ds(pl.multiple_of(slot * BLK, BLK), BLK)]
            elif kind == KIND_VEC:
                ref = sall.at[e, slot]
            else:
                ref = kall.at[e, slot, spans[kind]]
            return rcopy(ref, ref, e, group, kind, peer)

        def to_chip(e, kind):
            return gather(e, own, SEM_GATHER, kind, peer_chip)

        def to_core(e, kind):
            return gather(e, own, SEM_OWN, kind, peer_core)

        def forward(e, kind):
            return gather(e, 2 * core + (1 - chip), SEM_FWD, kind, peer_core)

        def stage2_q(e):
            core_reduce(e, KIND_Q).wait()
            for c in range(2):
                sq[e, c] = pq[e, 2 * core + c] + rq[e, c]
            chip_reduce(e, KIND_Q).start()

        def stage2_g(e, kind):
            if kind == KIND_DIAG:
                core_reduce(e, KIND_VEC).wait()
                sd[e] = pd[e] + rd[e]
                chip_reduce(e, KIND_VEC).start()
            core_reduce(e, kind).wait()
            for c in range(2):
                sg[e, c, spans[kind], :] = pg[e, 2 * core + c, spans[kind], :] + rg[e, c, spans[kind], :]
            chip_reduce(e, kind).start()

        def stage3_q(e):
            chip_reduce(e, KIND_Q).wait()
            full = sq[e, chip] + xq[e]
            qall[e, pl.ds(pl.multiple_of(own * BLK, BLK), BLK), :] = full.astype(BF16)
            to_chip(e, KIND_Q).start()
            to_core(e, KIND_Q).start()

        def stage3_g(e, kind):
            if kind == KIND_DIAG:
                chip_reduce(e, KIND_VEC).wait()
                dfull[...] = sd[e] + xd[e]
                first, last = 0, len(diag_blocks)
            else:
                first, last = len(diag_blocks), len(blocks)
            chip_reduce(e, kind).wait()
            row_id = lax.broadcasted_iota(jnp.int32, (piece, BLK), 0) + own * piece
            col_id = lax.broadcasted_iota(jnp.int32, (piece, BLK), 1)
            mine = row_id == col_id
            diag_cols = {}
            col_sums = [None] * nblk
            for index in range(first, last):
                i, j = blocks[index]
                rows = slice(index * piece, (index + 1) * piece)
                if i not in diag_cols:
                    diag_cols[i] = jnp.sum(jnp.where(mine, dfull[i:i + 1, :], 0.0), axis=1, keepdims=True)
                gram_rows = sg[e, chip, rows, :] + xg[e, rows, :]
                dist = jnp.maximum(diag_cols[i] + dfull[j:j + 1, :] - 2.0 * gram_rows, 0.0)
                kern = jnp.exp(-dist / bandwidth)
                kall[e, own, rows, :] = kern.astype(BF16)
                adds = [(j, kern)]
                if i != j:
                    adds.append((i, jnp.where(mine, jnp.sum(kern, axis=1, keepdims=True), 0.0)))
                for b, term in adds:
                    col_sums[b] = term if col_sums[b] is None else col_sums[b] + term
            for b in range(nblk):
                total = jnp.sum(col_sums[b], axis=0, keepdims=True)
                if kind == KIND_OFF:
                    total = total + sall[e, own, b:b + 1, :]
                sall[e, own, b:b + 1, :] = total
            for k in (kind,) if kind == KIND_DIAG else (kind, KIND_VEC):
                to_chip(e, k).start()
                to_core(e, k).start()

        def stage4(e, kinds):
            for kind in kinds:
                to_chip(e, kind).wait()
                forward(e, kind).start()

        def arrived(e, kind):
            to_core(e, kind).wait()
            forward(e, kind).wait()

        def stage5_q(e):
            arrived(e, KIND_Q)

        def stage5(e, kind):
            arrived(e, kind)
            for index, (i, j) in enumerate(blocks):
                if (index < len(diag_blocks)) != (kind == KIND_DIAG):
                    continue
                rows = slice(index * piece, (index + 1) * piece)
                block = jnp.concatenate([kall[e, o, rows, :].astype(F32) for o in range(nblk)], axis=0) * gain
                kfull[i * BLK:(i + 1) * BLK, j * BLK:(j + 1) * BLK] = block.astype(BF16)
                if i != j:
                    kfull[j * BLK:(j + 1) * BLK, i * BLK:(i + 1) * BLK] = block.T.astype(BF16)
            if kind == KIND_OFF:
                arrived(e, KIND_VEC)
                srow = sall[e, 0] + sall[e, 1] + sall[e, 2] + sall[e, 3]
                eye = (lax.broadcasted_iota(jnp.int32, (BLK, BLK), 0) == lax.broadcasted_iota(jnp.int32, (BLK, BLK), 1))
                for i in range(nblk):
                    col = jnp.sum(jnp.where(eye, srow[i:i + 1, :], 0.0), axis=1, keepdims=True)
                    scol[i * BLK:(i + 1) * BLK, :] = 1.0 + jnp.broadcast_to(col, (BLK, BLK)) * (gain * two_h)

        def round_inputs(e, ds, value):
            tb[:, ds] = value.astype(BF16)
            xb[:, ds] = (value - mu_ref[pl.ds(e, 1), ds]).astype(BF16)

        def mix(e, t):
            ds = tile_ds(t, MTILE)
            value = theta[e, :, ds]
            low = lax.dot_general(qall[e], u_ref[ds, :], TRANS_B, preferred_element_type=F32)
            centered = value - mu_ref[pl.ds(e, 1), ds]
            ybuf[:, ds] = (centered * (lam_ref[:, ds] + two_h) + (low + two_h * mu_ref[pl.ds(e, 1), ds])).astype(BF16)

        def drive(e, t):
            ds = tile_ds(t, DTILE)
            moved = jnp.dot(kfull[...], ybuf[:, ds], preferred_element_type=F32)
            new = theta[e, :, ds] * scol[:, 0:1] - moved
            theta[e, :, ds] = new
            return new

        def send_q(e):
            hk = num_local // 2

            @pl.when(feat >= 0)
            def _():
                part = [jnp.dot(xb[:, k * hk:(k + 1) * hk], u_ref[k * hk:(k + 1) * hk, :], preferred_element_type=F32) for k in range(2)]
                part = part[0] + part[1]
                for i in range(nblk):
                    pq[e, i] = part[i * BLK:(i + 1) * BLK, :]
            core_reduce(e, KIND_Q).start()

        def gram(e, kind):
            two = 2 * BLK
            hk = num_local // 2
            eye = (lax.broadcasted_iota(jnp.int32, (BLK, BLK), 0) == lax.broadcasted_iota(jnp.int32, (BLK, BLK), 1))

            def place(i, j, block):
                index = blocks.index((i, j))
                for o in range(nblk):
                    pg[e, o, index * piece:(index + 1) * piece, :] = block[o * piece:(o + 1) * piece]
                if i == j:
                    pd[e, i:i + 1, :] = jnp.sum(jnp.where(eye, block, 0.0), axis=0, keepdims=True)

            @pl.when(feat >= 0)
            def _():
                if kind == KIND_DIAG:
                    for half in range(2):
                        rows = tb[half * two:(half + 1) * two, :]
                        prod = lax.dot_general(rows, rows, TRANS_B, preferred_element_type=F32)
                        for i in range(2):
                            for j in range(i, 2):
                                place(2 * half + i, 2 * half + j, prod[i * BLK:(i + 1) * BLK, j * BLK:(j + 1) * BLK])
                else:
                    prod = [lax.dot_general(tb[0:two, k * hk:(k + 1) * hk], tb[two:2 * two, k * hk:(k + 1) * hk], TRANS_B,
                                            preferred_element_type=F32) for k in range(2)]
                    prod = prod[0] + prod[1]
                    for i in range(2):
                        for j in range(2):
                            place(i, 2 + j, prod[i * BLK:(i + 1) * BLK, j * BLK:(j + 1) * BLK])
            core_reduce(e, kind).start()
            if kind == KIND_DIAG:
                core_reduce(e, KIND_VEC).start()

        for e in range(2):
            pd[e] = jnp.zeros((8, BLK), F32)

        def loop(num, body):
            lax.fori_loop(0, num, lambda t, c: (body(t), c)[1], 0)

        def at(t, when, fn, *args):
            @pl.when(t == when)
            def _():
                fn(*args)

        def first_pass(e):
            def body(t):
                in_copy(e, t).wait()
                round_inputs(e, tile_ds(t), theta[e, :, tile_ds(t)])
            loop(num_tiles, body)

        for e in range(2):
            for t in range(num_tiles):
                in_copy(e, t).start()
        barrier = pltpu.get_barrier_semaphore()
        for peer in (peer_core, peer_chip):
            pl.semaphore_signal(barrier, inc=1, device_id=peer, device_id_type=pl.DeviceIdType.MESH)
        def send_gram(e):
            gram(e, KIND_DIAG)
            stage2_q(e)
            gram(e, KIND_OFF)

        first_pass(0)
        pl.semaphore_wait(barrier, 2)
        send_q(0)
        send_gram(0)
        first_pass(1)
        stage2_g(0, KIND_DIAG)
        stage2_g(0, KIND_OFF)
        send_q(1)
        stage3_q(0)
        gram(1, KIND_DIAG)
        stage2_q(1)
        gram(1, KIND_OFF)
        stage3_g(0, KIND_DIAG)
        stage3_g(0, KIND_OFF)
        stage4(0, (KIND_Q,))

        def finish_mix(e, o):
            stage5_q(e)
            if o is not None:
                stage4(e, (KIND_DIAG,))

            def mix_body(t):
                mix(e, t)
                if o is not None:
                    at(t, T2D, stage2_g, o, KIND_DIAG)
                    at(t, T4O, stage4, e, (KIND_OFF, KIND_VEC))
                    at(t, T2O, stage2_g, o, KIND_OFF)
            loop(num_local // MTILE, mix_body)
            if o is None:
                stage4(e, (KIND_DIAG, KIND_OFF, KIND_VEC))
            stage5(e, KIND_DIAG)
            stage5(e, KIND_OFF)

        def half_step(e, last):
            o = 1 - e
            finish_mix(e, o)

            def drive_body(t):
                new = drive(e, t)
                if not last:
                    round_inputs(e, tile_ds(t, DTILE), new)
                at(t, 0, stage3_q, o)
            loop(num_local // DTILE, drive_body)
            if S3 == 0:
                stage3_g(o, KIND_DIAG)
            if not last:
                send_q(e)
            stage4(o, (KIND_Q,))
            if S3 == 1:
                stage3_g(o, KIND_DIAG)
            stage3_g(o, KIND_OFF)
            if not last:
                send_gram(e)

        def steady(i, carry):
            half_step(i % 2, False)
            return carry

        lax.fori_loop(0, 2 * (NUM_STEPS - 1), steady, 0)
        half_step(0, True)
        finish_mix(1, None)

    def last_kernel(theta, ybuf, kfull, scol, out_hbm, new, out_sem):
        first = pltpu.make_async_copy(theta.at[0], out_hbm.at[0], out_sem.at[num_tiles])
        first.start()

        def out_copy(t):
            ds = pl.ds(pl.multiple_of(t * TILE, TILE), TILE)
            return pltpu.make_async_copy(new.at[:, ds], out_hbm.at[1, :, ds], out_sem.at[t])

        def body(t, carry):
            ds = pl.ds(pl.multiple_of(t * TILE, TILE), TILE)
            moved = jnp.dot(kfull[...], ybuf[:, ds], preferred_element_type=F32)
            new[:, ds] = theta[1, :, ds] * scol[:, 0:1] - moved
            out_copy(t).start()
            return carry

        lax.fori_loop(0, num_tiles, body, 0)
        first.wait()
        for t in range(num_tiles):
            out_copy(t).wait()

    def call(particles, target_mean, precision, low_factor):
        vm = pl.BlockSpec(memory_space=pltpu.VMEM)
        hbm = pl.BlockSpec(memory_space=pl.ANY)
        scratch = [
            pltpu.VMEM((num_part, num_local), BF16),
            pltpu.VMEM((num_part, num_local), BF16),
            pltpu.VMEM((2, nblk, BLK, BLK), F32),
            pltpu.VMEM((2, nblk, grow, BLK), F32),
            pltpu.VMEM((2, 8, BLK), F32),
            pltpu.VMEM((2, 2, BLK, BLK), F32),
            pltpu.VMEM((2, 2, grow, BLK), F32),
            pltpu.VMEM((2, 8, BLK), F32),
            pltpu.VMEM((2, 2, BLK, BLK), F32),
            pltpu.VMEM((2, 2, grow, BLK), F32),
            pltpu.VMEM((2, 8, BLK), F32),
            pltpu.VMEM((2, BLK, BLK), F32),
            pltpu.VMEM((2, grow, BLK), F32),
            pltpu.VMEM((2, 8, BLK), F32),
            pltpu.VMEM((8, BLK), F32),
            pltpu.VMEM((2, num_part, BLK), BF16),
            pltpu.VMEM((2, nblk, grow, BLK), BF16),
            pltpu.VMEM((2, nblk, 8, BLK), F32),
            pltpu.SemaphoreType.DMA((2, num_tiles)),
            pltpu.SemaphoreType.DMA((2, NUM_SEMS)),
            pltpu.SemaphoreType.DMA((2, NUM_SEMS)),
        ]
        state = pl.pallas_call(
            kernel,
            out_shape=(pltpu.VMEM(particles.shape, F32), pltpu.VMEM((num_part, num_local), BF16),
                       pltpu.VMEM((num_part, num_part), BF16), pltpu.VMEM((num_part, BLK), F32)),
            in_specs=[hbm, vm, vm, vm],
            out_specs=(vm, vm, vm, vm),
            scratch_shapes=scratch,
            compiler_params=pltpu.CompilerParams(
                collective_id=0, has_side_effects=True, vmem_limit_bytes=36 * 1024 * 1024),
            cost_estimate=pl.CostEstimate(flops=30 * 10**9, bytes_accessed=18 * 2**20, transcendentals=0),
        )(particles, target_mean, precision[None, :], low_factor)
        return pl.pallas_call(
            last_kernel,
            out_shape=jax.ShapeDtypeStruct(particles.shape, F32),
            in_specs=[vm, vm, vm, vm],
            out_specs=hbm,
            scratch_shapes=[pltpu.VMEM((num_part, num_local), F32), pltpu.SemaphoreType.DMA((num_tiles + 1,))],
            compiler_params=pltpu.CompilerParams(vmem_limit_bytes=10 * 1024 * 1024),
            cost_estimate=pl.CostEstimate(flops=2 * 10**9, bytes_accessed=16 * 2**20, transcendentals=0),
        )(*state)

    return call


def solution(mesh):
    feat_count = mesh.shape["feat"]
    data_spec = P("ens", None, "feat")

    def local_steps(particles, target_mean, precision, low_factor):
        num_part, num_local = particles.shape[1], particles.shape[2]
        call = build_kernel(num_part, num_local, num_local * feat_count)
        return call(particles, target_mean, precision, low_factor)

    return jax.shard_map(
        local_steps, mesh=mesh,
        in_specs=(data_spec, P("ens", "feat"), P(("ens", "feat")), P(("ens", "feat"), None)),
        out_specs=data_spec, check_vma=False)
```

```python
import jax
import jax.numpy as jnp
from jax import lax
from jax.experimental import pallas as pl
from jax.experimental.pallas import tpu as pltpu
from jax.sharding import PartitionSpec as P

NUM_STEPS = 3
BLK = 128
TILE = 1024
OUT_TILE = 512
MTILE = 2048
DTILE = 2048
T2D = 0
T4O = 0
T2O = 1
LTILE = 1024
L3D = 2
P2Q = 0
P2O = 0
F32 = jnp.float32
BF16 = jnp.bfloat16
TRANS_B = (((1,), (1,)), ((), ()))

SEM_CORE, SEM_CHIP, SEM_GATHER, SEM_OWN, SEM_FWD = range(5)
KIND_Q, KIND_DIAG, KIND_OFF, KIND_VEC = range(4)
NUM_KINDS = 4
NUM_SEMS = 5 * NUM_KINDS


def build_kernel(num_part, num_local, total_feat):
    nblk = num_part // BLK
    num_tiles = num_local // TILE
    bandwidth = 2.0 * total_feat
    step_size = 0.25 * total_feat
    two_h = 2.0 / bandwidth
    gain = step_size / num_part
    piece = BLK // nblk
    diag_blocks = ((0, 1, True), (2, 3, True), (0, 1, False), (2, 3, False))
    off_blocks = ((0, 2, False), (0, 3, False), (1, 2, False), (1, 3, False))
    blocks = diag_blocks + off_blocks
    grow = piece * len(blocks)
    split = piece * len(diag_blocks)
    spans = {KIND_DIAG: pl.ds(0, split), KIND_OFF: pl.ds(split, grow - split)}

    def kernel(th_hbm, mu_hbm, lam_hbm, u_hbm, theta, ybuf, kfull, scol,
               tb,
               pq, pg, pd, rq, rg, rd, sq, sg, sd, xq, xg, xd, dfull,
               qall, kall, sall,
               mu_ref, lam_ref, u_ref, in_sem, par_sem, send_sem, recv_sem):
        feat = lax.axis_index("feat")
        chip = feat // 2
        core = feat % 2
        own = 2 * core + chip
        peer_core = {"feat": 2 * chip + (1 - core)}
        peer_chip = {"feat": 2 * (1 - chip) + core}

        def rcopy(src, dst, e, group, kind, peer):
            idx = group * NUM_KINDS + kind
            return pltpu.make_async_remote_copy(
                src_ref=src, dst_ref=dst, send_sem=send_sem.at[e, idx], recv_sem=recv_sem.at[e, idx],
                device_id=peer, device_id_type=pl.DeviceIdType.MESH)

        def tile_ds(t, size=TILE):
            return pl.ds(pl.multiple_of(t * size, size), size)

        def in_copy(e, t):
            return pltpu.make_async_copy(th_hbm.at[e, :, tile_ds(t)], theta.at[e, :, tile_ds(t)], in_sem.at[e, t])

        def core_reduce(e, kind):
            if kind == KIND_Q:
                src, dst = pq.at[e, pl.ds(2 * (1 - core), 2)], rq.at[e]
            elif kind == KIND_VEC:
                src, dst = pd.at[e], rd.at[e]
            else:
                src, dst = pg.at[e, pl.ds(2 * (1 - core), 2), spans[kind]], rg.at[e, :, spans[kind]]
            return rcopy(src, dst, e, SEM_CORE, kind, peer_core)

        def chip_reduce(e, kind):
            if kind == KIND_Q:
                src, dst = sq.at[e, 1 - chip], xq.at[e]
            elif kind == KIND_VEC:
                src, dst = sd.at[e], xd.at[e]
            else:
                src, dst = sg.at[e, 1 - chip, spans[kind]], xg.at[e, spans[kind]]
            return rcopy(src, dst, e, SEM_CHIP, kind, peer_chip)

        def gather(e, slot, group, kind, peer):
            if kind == KIND_Q:
                ref = qall.at[e, pl.ds(pl.multiple_of(slot * BLK, BLK), BLK)]
            elif kind == KIND_VEC:
                ref = sall.at[e, slot]
            else:
                ref = kall.at[e, slot, spans[kind]]
            return rcopy(ref, ref, e, group, kind, peer)

        def to_chip(e, kind):
            return gather(e, own, SEM_GATHER, kind, peer_chip)

        def to_core(e, kind):
            return gather(e, own, SEM_OWN, kind, peer_core)

        def forward(e, kind):
            return gather(e, 2 * core + (1 - chip), SEM_FWD, kind, peer_core)

        def stage2_q(e):
            core_reduce(e, KIND_Q).wait()
            for c in range(2):
                sq[e, c] = pq[e, 2 * core + c] + rq[e, c]
            chip_reduce(e, KIND_Q).start()

        def stage2_g(e, kind):
            if kind == KIND_DIAG:
                core_reduce(e, KIND_VEC).wait()
                sd[e] = pd[e] + rd[e]
                chip_reduce(e, KIND_VEC).start()
            core_reduce(e, kind).wait()
            for c in range(2):
                sg[e, c, spans[kind], :] = pg[e, 2 * core + c, spans[kind], :] + rg[e, c, spans[kind], :]
            chip_reduce(e, kind).start()

        def stage3_q(e):
            chip_reduce(e, KIND_Q).wait()
            full = sq[e, chip] + xq[e]
            qall[e, pl.ds(pl.multiple_of(own * BLK, BLK), BLK), :] = full.astype(BF16)
            to_chip(e, KIND_Q).start()
            to_core(e, KIND_Q).start()

        def kernel_of(norm, value):
            return jnp.exp(-jnp.maximum(norm - 2.0 * value, 0.0) / bandwidth)

        def kernel_diag(b):
            norm = dfull[b:b + 1, :]
            return kernel_of(norm + norm, norm)

        def stage3_g(e, kind):
            if kind == KIND_DIAG:
                chip_reduce(e, KIND_VEC).wait()
                dfull[...] = sd[e] + xd[e]
                first, last = 0, len(diag_blocks)
            else:
                first, last = len(diag_blocks), len(blocks)
            chip_reduce(e, kind).wait()
            row_id = lax.broadcasted_iota(jnp.int32, (piece, BLK), 0) + own * piece
            col_id = lax.broadcasted_iota(jnp.int32, (piece, BLK), 1)
            mine = row_id == col_id
            upper, lower = row_id < col_id, row_id > col_id
            diag_cols = {}
            col_sums = [None] * nblk

            def diag_row(b):
                return dfull[b:b + 1, :]

            def diag_col(b):
                if b not in diag_cols:
                    diag_cols[b] = jnp.sum(jnp.where(mine, diag_row(b), 0.0), axis=1, keepdims=True)
                return diag_cols[b]

            def add(b, term):
                col_sums[b] = term if col_sums[b] is None else col_sums[b] + term

            def add_rows(b, term):
                add(b, jnp.where(mine, jnp.sum(term, axis=1, keepdims=True), 0.0))

            for index in range(first, last):
                i, j, packed = blocks[index]
                rows = slice(index * piece, (index + 1) * piece)
                gram_rows = sg[e, chip, rows, :] + xg[e, rows, :]
                if packed:
                    norm = jnp.where(lower, diag_col(j) + diag_row(j), diag_col(i) + diag_row(i))
                else:
                    norm = diag_col(i) + diag_row(j)
                kern = kernel_of(norm, gram_rows)
                kall[e, own, rows, :] = (kern * gain).astype(BF16)
                if packed:
                    kern_up, kern_low = jnp.where(upper, kern, 0.0), jnp.where(lower, kern, 0.0)
                    add(i, jnp.where(lower, 0.0, kern))
                    add_rows(i, kern_up)
                    add(j, kern_low + jnp.where(mine, kernel_diag(j), 0.0))
                    add_rows(j, kern_low)
                else:
                    add(j, kern)
                    add_rows(i, kern)
            for b in range(nblk):
                total = jnp.sum(col_sums[b], axis=0, keepdims=True)
                if kind == KIND_OFF:
                    total = total + sall[e, own, b:b + 1, :]
                sall[e, own, b:b + 1, :] = total
            for k in (kind,) if kind == KIND_DIAG else (kind, KIND_VEC):
                to_chip(e, k).start()
                to_core(e, k).start()

        def stage4(e, kinds):
            for kind in kinds:
                to_chip(e, kind).wait()
                forward(e, kind).start()

        def arrived(e, kind):
            to_core(e, kind).wait()
            forward(e, kind).wait()

        def stage5_q(e):
            arrived(e, KIND_Q)

        def stage5(e, kind):
            arrived(e, kind)
            row_id = lax.broadcasted_iota(jnp.int32, (BLK, BLK), 0)
            col_id = lax.broadcasted_iota(jnp.int32, (BLK, BLK), 1)

            def put(i, j, value):
                kfull[i * BLK:(i + 1) * BLK, j * BLK:(j + 1) * BLK] = value.astype(BF16)

            for index, (i, j, packed) in enumerate(blocks):
                if (index < len(diag_blocks)) != (kind == KIND_DIAG):
                    continue
                rows = slice(index * piece, (index + 1) * piece)
                block = jnp.concatenate([kall[e, o, rows, :].astype(F32) for o in range(nblk)], axis=0)
                flipped = block.T
                if packed:
                    put(i, i, jnp.where(row_id <= col_id, block, flipped))
                    rest = jnp.where(row_id < col_id, flipped, (kernel_diag(j) * gain).astype(BF16).astype(F32))
                    put(j, j, jnp.where(row_id > col_id, block, rest))
                else:
                    put(i, j, block)
                    put(j, i, flipped)
            if kind == KIND_OFF:
                arrived(e, KIND_VEC)
                srow = sall[e, 0] + sall[e, 1] + sall[e, 2] + sall[e, 3]
                eye = (lax.broadcasted_iota(jnp.int32, (BLK, BLK), 0) == lax.broadcasted_iota(jnp.int32, (BLK, BLK), 1))
                for i in range(nblk):
                    col = jnp.sum(jnp.where(eye, srow[i:i + 1, :], 0.0), axis=1, keepdims=True)
                    scol[i * BLK:(i + 1) * BLK, :] = 1.0 + jnp.broadcast_to(col, (BLK, BLK)) * (gain * two_h)

        def round_inputs(e, ds, value):
            tb[:, ds] = value.astype(BF16)

        def mix(e, t):
            ds = tile_ds(t, MTILE)
            value = theta[e, :, ds]
            low = lax.dot_general(qall[e], u_ref[ds, :], TRANS_B, preferred_element_type=F32)
            centered = value - mu_ref[pl.ds(e, 1), ds]
            ybuf[:, ds] = (centered * (lam_ref[:, ds] + two_h) + (low + two_h * mu_ref[pl.ds(e, 1), ds])).astype(BF16)

        def drive(e, ds):
            moved = jnp.dot(kfull[...], ybuf[:, ds], preferred_element_type=F32)
            new = theta[e, :, ds] * scol[:, 0:1] - moved
            theta[e, :, ds] = new
            return new

        def q_dot(e, ds_a, ds_b):
            parts = [jnp.dot((theta[e, :, d] - mu_ref[pl.ds(e, 1), d]).astype(BF16), u_ref[d, :], preferred_element_type=F32) for d in (ds_a, ds_b)]
            return parts[0] + parts[1]

        def gram_dots(kind, ds_all, ds_a, ds_b):
            two = 2 * BLK
            out = {}
            if kind == KIND_DIAG:
                for half in range(2):
                    rows = tb[half * two:(half + 1) * two, ds_all]
                    prod = lax.dot_general(rows, rows, TRANS_B, preferred_element_type=F32)
                    for i in range(2):
                        for j in range(i, 2):
                            out[2 * half + i, 2 * half + j] = prod[i * BLK:(i + 1) * BLK, j * BLK:(j + 1) * BLK]
            else:
                prod = [lax.dot_general(tb[0:two, d], tb[two:2 * two, d], TRANS_B, preferred_element_type=F32)
                        for d in (ds_a, ds_b)]
                prod = prod[0] + prod[1]
                for i in range(2):
                    for j in range(2):
                        out[i, 2 + j] = prod[i * BLK:(i + 1) * BLK, j * BLK:(j + 1) * BLK]
            return out

        def put_q(e, value):
            for i in range(nblk):
                pq[e, i] = value[i * BLK:(i + 1) * BLK, :]

        def put_gram(e, kind, out, add):
            row_id = lax.broadcasted_iota(jnp.int32, (BLK, BLK), 0)
            col_id = lax.broadcasted_iota(jnp.int32, (BLK, BLK), 1)
            for index, (i, j, packed) in enumerate(blocks):
                if (index < len(diag_blocks)) != (kind == KIND_DIAG):
                    continue
                block = jnp.where(row_id <= col_id, out[i, i], out[j, j]) if packed else out[i, j]
                for o in range(nblk):
                    rows = slice(index * piece, (index + 1) * piece)
                    term = block[o * piece:(o + 1) * piece]
                    pg[e, o, rows, :] = pg[e, o, rows, :] + term if add else term
            if kind == KIND_DIAG:
                for i in range(nblk):
                    term = jnp.sum(jnp.where(row_id == col_id, out[i, i], 0.0), axis=0, keepdims=True)
                    pd[e, i:i + 1, :] = pd[e, i:i + 1, :] + term if add else term

        def first_chunk(e, c):
            half = TILE // 2
            in_copy(e, c).wait()
            round_inputs(e, tile_ds(c), theta[e, :, tile_ds(c)])
            start = pl.multiple_of(c * TILE, TILE)
            ds_a, ds_b = pl.ds(start, half), pl.ds(start + half, half)
            for kind in (KIND_DIAG, KIND_OFF):
                put_gram(e, kind, gram_dots(kind, tile_ds(c), ds_a, ds_b), True)

        def send(e, kinds):
            for kind in kinds:
                core_reduce(e, kind).start()

        half_a, half_b, whole = pl.ds(0, num_local // 2), pl.ds(num_local // 2, num_local // 2), pl.ds(0, num_local)

        def sums_1(e):
            @pl.when(feat >= 0)
            def _():
                put_q(e, q_dot(e, half_a, half_b))
            send(e, (KIND_Q,))

        def sums_2(e):
            @pl.when(feat >= 0)
            def _():
                put_gram(e, KIND_DIAG, gram_dots(KIND_DIAG, whole, half_a, half_b), False)
            send(e, (KIND_VEC, KIND_DIAG))
            stage2_q(e)

            @pl.when(feat >= 0)
            def _():
                put_gram(e, KIND_OFF, gram_dots(KIND_OFF, whole, half_a, half_b), False)
            send(e, (KIND_OFF,))

        for e in range(2):
            pd[e] = jnp.zeros((8, BLK), F32)

        def loop(num, body):
            lax.fori_loop(0, num, lambda t, c: (body(t), c)[1], 0)

        def at(t, when, fn, *args):
            @pl.when(t == when)
            def _():
                fn(*args)

        def par_copy(index):
            src, dst = ((mu_hbm, mu_ref), (lam_hbm, lam_ref), (u_hbm, u_ref))[index]
            return pltpu.make_async_copy(src, dst, par_sem.at[index])

        for c in range(num_tiles):
            in_copy(0, c).start()
        for index in range(3):
            par_copy(index).start()
        for c in range(num_tiles):
            in_copy(1, c).start()
        barrier = pltpu.get_barrier_semaphore()
        for peer in (peer_core, peer_chip):
            pl.semaphore_signal(barrier, inc=1, device_id=peer, device_id_type=pl.DeviceIdType.MESH)
        def send_gram(e):
            gram(e, KIND_DIAG)
            stage2_q(e)
            gram(e, KIND_OFF)

        for e in range(2):
            pg[e] = jnp.zeros((nblk, grow, BLK), F32)
        loop(num_tiles, lambda c: first_chunk(0, c))
        par_copy(0).wait()
        par_copy(2).wait()
        pl.semaphore_wait(barrier, 2)
        send(0, (KIND_VEC, KIND_DIAG, KIND_OFF))
        sums_1(0)
        stage2_g(0, KIND_DIAG)

        def second_pass(c):
            first_chunk(1, c)
            at(c, P2Q, stage2_q, 0)
            at(c, P2O, stage2_g, 0, KIND_OFF)
        loop(num_tiles, second_pass)
        send(1, (KIND_VEC, KIND_DIAG, KIND_OFF))
        stage3_g(0, KIND_DIAG)
        stage3_q(0)
        sums_1(1)
        stage3_g(0, KIND_OFF)
        stage4(0, (KIND_Q,))
        stage2_q(1)
        par_copy(1).wait()

        def finish_mix(e, o):
            stage5_q(e)
            stage4(e, (KIND_DIAG,))

            def mix_body(t):
                mix(e, t)
                at(t, T4O, stage4, e, (KIND_OFF, KIND_VEC))
                if o is not None:
                    at(t, T2D, stage2_g, o, KIND_DIAG)
                    at(t, T2O, stage2_g, o, KIND_OFF)
            loop(num_local // MTILE, mix_body)
            stage5(e, KIND_DIAG)
            stage5(e, KIND_OFF)

        def half_step(e):
            o = 1 - e
            finish_mix(e, o)

            def drive_body(t):
                round_inputs(e, tile_ds(t, DTILE), drive(e, tile_ds(t, DTILE)))
                at(t, 0, stage3_q, o)
            loop(num_local // DTILE, drive_body)
            stage3_g(o, KIND_DIAG)
            sums_1(e)
            stage4(o, (KIND_Q,))
            stage3_g(o, KIND_OFF)
            sums_2(e)

        def last_half_step():
            finish_mix(0, 1)

            stage3_q(1)

            def drive_body(t):
                drive(0, tile_ds(t, LTILE))
                at(t, L3D, stage3_g, 1, KIND_DIAG)
            loop(num_local // LTILE, drive_body)
            stage3_g(1, KIND_OFF)
            stage4(1, (KIND_Q,))
            finish_mix(1, None)

        def steady(i, carry):
            half_step(i % 2)
            return carry

        lax.fori_loop(0, 2 * (NUM_STEPS - 1), steady, 0)
        last_half_step()

    out_tiles = num_local // OUT_TILE

    def last_kernel(theta, ybuf, kfull, scol, out_hbm, new, out_sem):
        first = pltpu.make_async_copy(theta.at[0], out_hbm.at[0], out_sem.at[out_tiles])
        first.start()

        def out_copy(t):
            ds = pl.ds(pl.multiple_of(t * OUT_TILE, OUT_TILE), OUT_TILE)
            return pltpu.make_async_copy(new.at[:, ds], out_hbm.at[1, :, ds], out_sem.at[t])

        def body(t, carry):
            ds = pl.ds(pl.multiple_of(t * OUT_TILE, OUT_TILE), OUT_TILE)
            moved = jnp.dot(kfull[...], ybuf[:, ds], preferred_element_type=F32)
            new[:, ds] = theta[1, :, ds] * scol[:, 0:1] - moved
            out_copy(t).start()
            return carry

        lax.fori_loop(0, out_tiles, body, 0)
        first.wait()
        for t in range(out_tiles):
            out_copy(t).wait()

    def call(particles, target_mean, precision, low_factor):
        vm = pl.BlockSpec(memory_space=pltpu.VMEM)
        hbm = pl.BlockSpec(memory_space=pltpu.HBM)
        scratch = [
            pltpu.VMEM((num_part, num_local), BF16),
            pltpu.VMEM((2, nblk, BLK, BLK), F32),
            pltpu.VMEM((2, nblk, grow, BLK), F32),
            pltpu.VMEM((2, 8, BLK), F32),
            pltpu.VMEM((2, 2, BLK, BLK), F32),
            pltpu.VMEM((2, 2, grow, BLK), F32),
            pltpu.VMEM((2, 8, BLK), F32),
            pltpu.VMEM((2, 2, BLK, BLK), F32),
            pltpu.VMEM((2, 2, grow, BLK), F32),
            pltpu.VMEM((2, 8, BLK), F32),
            pltpu.VMEM((2, BLK, BLK), F32),
            pltpu.VMEM((2, grow, BLK), F32),
            pltpu.VMEM((2, 8, BLK), F32),
            pltpu.VMEM((8, BLK), F32),
            pltpu.VMEM((2, num_part, BLK), BF16),
            pltpu.VMEM((2, nblk, grow, BLK), BF16),
            pltpu.VMEM((2, nblk, 8, BLK), F32),
            pltpu.VMEM((2, num_local), F32),
            pltpu.VMEM((1, num_local), F32),
            pltpu.VMEM((num_local, BLK), BF16),
            pltpu.SemaphoreType.DMA((2, num_tiles)),
            pltpu.SemaphoreType.DMA((3,)),
            pltpu.SemaphoreType.DMA((2, NUM_SEMS)),
            pltpu.SemaphoreType.DMA((2, NUM_SEMS)),
        ]
        state = pl.pallas_call(
            kernel,
            out_shape=(pltpu.VMEM(particles.shape, F32), pltpu.VMEM((num_part, num_local), BF16),
                       pltpu.VMEM((num_part, num_part), BF16), pltpu.VMEM((num_part, BLK), F32)),
            in_specs=[hbm, hbm, hbm, hbm],
            out_specs=(vm, vm, vm, vm),
            scratch_shapes=scratch,
            compiler_params=pltpu.CompilerParams(
                collective_id=0, has_side_effects=True, vmem_limit_bytes=36 * 1024 * 1024),
            cost_estimate=pl.CostEstimate(flops=30 * 10**9, bytes_accessed=18 * 2**20, transcendentals=0),
        )(particles, target_mean, precision[None, :], low_factor)
        return pl.pallas_call(
            last_kernel,
            out_shape=jax.ShapeDtypeStruct(particles.shape, F32),
            in_specs=[vm, vm, vm, vm],
            out_specs=hbm,
            scratch_shapes=[pltpu.VMEM((num_part, num_local), F32), pltpu.SemaphoreType.DMA((out_tiles + 1,))],
            compiler_params=pltpu.CompilerParams(vmem_limit_bytes=10 * 1024 * 1024),
            cost_estimate=pl.CostEstimate(flops=2 * 10**9, bytes_accessed=16 * 2**20, transcendentals=0),
        )(*state)

    return call


def solution(mesh):
    feat_count = mesh.shape["feat"]
    data_spec = P("ens", None, "feat")

    def local_steps(particles, target_mean, precision, low_factor):
        num_part, num_local = particles.shape[1], particles.shape[2]
        call = build_kernel(num_part, num_local, num_local * feat_count)
        return call(particles, target_mean, precision, low_factor)

    return jax.shard_map(
        local_steps, mesh=mesh,
        in_specs=(data_spec, P("ens", "feat"), P(("ens", "feat")), P(("ens", "feat"), None)),
        out_specs=data_spec, check_vma=False)
```

```python
import jax
import jax.numpy as jnp
from jax import lax
from jax.experimental import pallas as pl
from jax.experimental.pallas import tpu as pltpu
from jax.sharding import PartitionSpec as P

NUM_STEPS = 3
BLK = 128
TILE = 1024
OUT_TILE = 512
MTILE = 2048
DTILE = 2048
T2D = 0
T4O = 0
T2O = 1
LTILE = 1024
L3D = 2
P2Q = 0
P2O = 0
F32 = jnp.float32
BF16 = jnp.bfloat16
TRANS_B = (((1,), (1,)), ((), ()))

SEM_CORE, SEM_CHIP, SEM_GATHER, SEM_OWN, SEM_FWD = range(5)
KIND_Q, KIND_DIAG, KIND_OFF, KIND_VEC = range(4)
NUM_KINDS = 4
DIRECT = (KIND_DIAG, KIND_OFF, KIND_VEC)
NUM_SEMS = 5 * NUM_KINDS


def build_kernel(num_part, num_local, total_feat):
    nblk = num_part // BLK
    num_tiles = num_local // TILE
    bandwidth = 2.0 * total_feat
    step_size = 0.25 * total_feat
    two_h = 2.0 / bandwidth
    gain = step_size / num_part
    piece = BLK // nblk
    diag_blocks = ((0, 1, True), (2, 3, True), (0, 1, False), (2, 3, False))
    off_blocks = ((0, 2, False), (0, 3, False), (1, 2, False), (1, 3, False))
    blocks = diag_blocks + off_blocks
    grow = piece * len(blocks)
    split = piece * len(diag_blocks)
    spans = {KIND_DIAG: pl.ds(0, split), KIND_OFF: pl.ds(split, grow - split)}

    def kernel(th_hbm, mu_hbm, lam_hbm, u_hbm, theta, ybuf, kfull, scol,
               tb,
               pq, pg, pd, rq, rg, rd, sq, sg, sd, xq, xg, xd, dfull,
               qall, kall, sall,
               mu_ref, lam_ref, u_ref, in_sem, par_sem, send_sem, recv_sem):
        feat = lax.axis_index("feat")
        chip = feat // 2
        core = feat % 2
        own = 2 * core + chip
        peer_core = {"feat": 2 * chip + (1 - core)}
        peer_chip = {"feat": 2 * (1 - chip) + core}
        peer_cross = {"feat": 2 * (1 - chip) + (1 - core)}

        def rcopy(src, dst, e, group, kind, peer):
            idx = group * NUM_KINDS + kind
            return pltpu.make_async_remote_copy(
                src_ref=src, dst_ref=dst, send_sem=send_sem.at[e, idx], recv_sem=recv_sem.at[e, idx],
                device_id=peer, device_id_type=pl.DeviceIdType.MESH)

        def tile_ds(t, size=TILE):
            return pl.ds(pl.multiple_of(t * size, size), size)

        def in_copy(e, t):
            return pltpu.make_async_copy(th_hbm.at[e, :, tile_ds(t)], theta.at[e, :, tile_ds(t)], in_sem.at[e, t])

        def core_reduce(e, kind):
            if kind == KIND_Q:
                src, dst = pq.at[e, pl.ds(2 * (1 - core), 2)], rq.at[e]
            elif kind == KIND_VEC:
                src, dst = pd.at[e], rd.at[e]
            else:
                src, dst = pg.at[e, pl.ds(2 * (1 - core), 2), spans[kind]], rg.at[e, :, spans[kind]]
            return rcopy(src, dst, e, SEM_CORE, kind, peer_core)

        def chip_reduce(e, kind):
            if kind == KIND_Q:
                src, dst = sq.at[e, 1 - chip], xq.at[e]
            elif kind == KIND_VEC:
                src, dst = sd.at[e], xd.at[e]
            else:
                src, dst = sg.at[e, 1 - chip, spans[kind]], xg.at[e, spans[kind]]
            return rcopy(src, dst, e, SEM_CHIP, kind, peer_chip)

        def gather(e, slot, group, kind, peer):
            if kind == KIND_Q:
                ref = qall.at[e, pl.ds(pl.multiple_of(slot * BLK, BLK), BLK)]
            elif kind == KIND_VEC:
                ref = sall.at[e, slot]
            else:
                ref = kall.at[e, slot, spans[kind]]
            return rcopy(ref, ref, e, group, kind, peer)

        def to_chip(e, kind):
            return gather(e, own, SEM_GATHER, kind, peer_chip)

        def to_core(e, kind):
            return gather(e, own, SEM_OWN, kind, peer_core)

        def to_cross(e, kind):
            return gather(e, own, SEM_FWD, kind, peer_cross)

        def start_gather(e, kind):
            to_chip(e, kind).start()
            if kind in DIRECT:
                to_cross(e, kind).start()
            to_core(e, kind).start()

        def forward(e, kind):
            return gather(e, 2 * core + (1 - chip), SEM_FWD, kind, peer_core)

        def stage2_q(e):
            core_reduce(e, KIND_Q).wait()
            for c in range(2):
                sq[e, c] = pq[e, 2 * core + c] + rq[e, c]
            chip_reduce(e, KIND_Q).start()

        def stage2_g(e, kind):
            if kind == KIND_DIAG:
                core_reduce(e, KIND_VEC).wait()
                sd[e] = pd[e] + rd[e]
                chip_reduce(e, KIND_VEC).start()
            core_reduce(e, kind).wait()
            for c in range(2):
                sg[e, c, spans[kind], :] = pg[e, 2 * core + c, spans[kind], :] + rg[e, c, spans[kind], :]
            chip_reduce(e, kind).start()

        def stage3_q(e):
            chip_reduce(e, KIND_Q).wait()
            full = sq[e, chip] + xq[e]
            qall[e, pl.ds(pl.multiple_of(own * BLK, BLK), BLK), :] = full.astype(BF16)
            start_gather(e, KIND_Q)

        def kernel_of(norm, value):
            return jnp.exp(-jnp.maximum(norm - 2.0 * value, 0.0) / bandwidth)

        def kernel_diag(b):
            norm = dfull[b:b + 1, :]
            return kernel_of(norm + norm, norm)

        def stage3_g(e, kind):
            if kind == KIND_DIAG:
                chip_reduce(e, KIND_VEC).wait()
                dfull[...] = sd[e] + xd[e]
                first, last = 0, len(diag_blocks)
            else:
                first, last = len(diag_blocks), len(blocks)
            chip_reduce(e, kind).wait()
            row_id = lax.broadcasted_iota(jnp.int32, (piece, BLK), 0) + own * piece
            col_id = lax.broadcasted_iota(jnp.int32, (piece, BLK), 1)
            mine = row_id == col_id
            upper, lower = row_id < col_id, row_id > col_id
            diag_cols = {}
            col_sums = [None] * nblk

            def diag_row(b):
                return dfull[b:b + 1, :]

            def diag_col(b):
                if b not in diag_cols:
                    diag_cols[b] = jnp.sum(jnp.where(mine, diag_row(b), 0.0), axis=1, keepdims=True)
                return diag_cols[b]

            def add(b, term):
                col_sums[b] = term if col_sums[b] is None else col_sums[b] + term

            def add_rows(b, term):
                add(b, jnp.where(mine, jnp.sum(term, axis=1, keepdims=True), 0.0))

            for index in range(first, last):
                i, j, packed = blocks[index]
                rows = slice(index * piece, (index + 1) * piece)
                gram_rows = sg[e, chip, rows, :] + xg[e, rows, :]
                if packed:
                    norm = jnp.where(lower, diag_col(j) + diag_row(j), diag_col(i) + diag_row(i))
                else:
                    norm = diag_col(i) + diag_row(j)
                kern = kernel_of(norm, gram_rows)
                kall[e, own, rows, :] = (kern * gain).astype(BF16)
                if packed:
                    kern_up, kern_low = jnp.where(upper, kern, 0.0), jnp.where(lower, kern, 0.0)
                    add(i, jnp.where(lower, 0.0, kern))
                    add_rows(i, kern_up)
                    add(j, kern_low + jnp.where(mine, kernel_diag(j), 0.0))
                    add_rows(j, kern_low)
                else:
                    add(j, kern)
                    add_rows(i, kern)
            for b in range(nblk):
                total = jnp.sum(col_sums[b], axis=0, keepdims=True)
                if kind == KIND_OFF:
                    total = total + sall[e, own, b:b + 1, :]
                sall[e, own, b:b + 1, :] = total
            for k in (kind,) if kind == KIND_DIAG else (kind, KIND_VEC):
                start_gather(e, k)

        def stage4(e, kinds):
            for kind in kinds:
                if kind not in DIRECT:
                    to_chip(e, kind).wait()
                    forward(e, kind).start()

        def arrived(e, kind):
            to_core(e, kind).wait()
            if kind in DIRECT:
                to_chip(e, kind).wait()
                to_cross(e, kind).wait()
            else:
                forward(e, kind).wait()

        def stage5_q(e):
            arrived(e, KIND_Q)

        def stage5(e, kind):
            arrived(e, kind)
            row_id = lax.broadcasted_iota(jnp.int32, (BLK, BLK), 0)
            col_id = lax.broadcasted_iota(jnp.int32, (BLK, BLK), 1)

            def put(i, j, value):
                kfull[i * BLK:(i + 1) * BLK, j * BLK:(j + 1) * BLK] = value.astype(BF16)

            for index, (i, j, packed) in enumerate(blocks):
                if (index < len(diag_blocks)) != (kind == KIND_DIAG):
                    continue
                rows = slice(index * piece, (index + 1) * piece)
                block = jnp.concatenate([kall[e, o, rows, :].astype(F32) for o in range(nblk)], axis=0)
                flipped = block.T
                if packed:
                    put(i, i, jnp.where(row_id <= col_id, block, flipped))
                    rest = jnp.where(row_id < col_id, flipped, (kernel_diag(j) * gain).astype(BF16).astype(F32))
                    put(j, j, jnp.where(row_id > col_id, block, rest))
                else:
                    put(i, j, block)
                    put(j, i, flipped)
            if kind == KIND_OFF:
                arrived(e, KIND_VEC)
                srow = sall[e, 0] + sall[e, 1] + sall[e, 2] + sall[e, 3]
                eye = (lax.broadcasted_iota(jnp.int32, (BLK, BLK), 0) == lax.broadcasted_iota(jnp.int32, (BLK, BLK), 1))
                for i in range(nblk):
                    col = jnp.sum(jnp.where(eye, srow[i:i + 1, :], 0.0), axis=1, keepdims=True)
                    scol[i * BLK:(i + 1) * BLK, :] = 1.0 + jnp.broadcast_to(col, (BLK, BLK)) * (gain * two_h)

        def round_inputs(e, ds, value):
            tb[:, ds] = value.astype(BF16)

        def mix(e, t):
            ds = tile_ds(t, MTILE)
            value = theta[e, :, ds]
            low = lax.dot_general(qall[e], u_ref[ds, :], TRANS_B, preferred_element_type=F32)
            centered = value - mu_ref[pl.ds(e, 1), ds]
            ybuf[:, ds] = (centered * (lam_ref[:, ds] + two_h) + (low + two_h * mu_ref[pl.ds(e, 1), ds])).astype(BF16)

        def drive(e, ds):
            moved = jnp.dot(kfull[...], ybuf[:, ds], preferred_element_type=F32)
            new = theta[e, :, ds] * scol[:, 0:1] - moved
            theta[e, :, ds] = new
            return new

        def q_dot(e, ds_a, ds_b):
            parts = [jnp.dot((theta[e, :, d] - mu_ref[pl.ds(e, 1), d]).astype(BF16), u_ref[d, :], preferred_element_type=F32) for d in (ds_a, ds_b)]
            return parts[0] + parts[1]

        def gram_dots(kind, ds_all, ds_a, ds_b):
            two = 2 * BLK
            out = {}
            if kind == KIND_DIAG:
                for half in range(2):
                    rows = tb[half * two:(half + 1) * two, ds_all]
                    prod = lax.dot_general(rows, rows, TRANS_B, preferred_element_type=F32)
                    for i in range(2):
                        for j in range(i, 2):
                            out[2 * half + i, 2 * half + j] = prod[i * BLK:(i + 1) * BLK, j * BLK:(j + 1) * BLK]
            else:
                prod = [lax.dot_general(tb[0:two, d], tb[two:2 * two, d], TRANS_B, preferred_element_type=F32)
                        for d in (ds_a, ds_b)]
                prod = prod[0] + prod[1]
                for i in range(2):
                    for j in range(2):
                        out[i, 2 + j] = prod[i * BLK:(i + 1) * BLK, j * BLK:(j + 1) * BLK]
            return out

        def put_q(e, value):
            for i in range(nblk):
                pq[e, i] = value[i * BLK:(i + 1) * BLK, :]

        def put_gram(e, kind, out, add):
            row_id = lax.broadcasted_iota(jnp.int32, (BLK, BLK), 0)
            col_id = lax.broadcasted_iota(jnp.int32, (BLK, BLK), 1)
            for index, (i, j, packed) in enumerate(blocks):
                if (index < len(diag_blocks)) != (kind == KIND_DIAG):
                    continue
                block = jnp.where(row_id <= col_id, out[i, i], out[j, j]) if packed else out[i, j]
                for o in range(nblk):
                    rows = slice(index * piece, (index + 1) * piece)
                    term = block[o * piece:(o + 1) * piece]
                    pg[e, o, rows, :] = pg[e, o, rows, :] + term if add else term
            if kind == KIND_DIAG:
                for i in range(nblk):
                    term = jnp.sum(jnp.where(row_id == col_id, out[i, i], 0.0), axis=0, keepdims=True)
                    pd[e, i:i + 1, :] = pd[e, i:i + 1, :] + term if add else term

        def first_chunk(e, c):
            half = TILE // 2
            in_copy(e, c).wait()
            round_inputs(e, tile_ds(c), theta[e, :, tile_ds(c)])
            start = pl.multiple_of(c * TILE, TILE)
            ds_a, ds_b = pl.ds(start, half), pl.ds(start + half, half)
            for kind in (KIND_DIAG, KIND_OFF):
                put_gram(e, kind, gram_dots(kind, tile_ds(c), ds_a, ds_b), True)

        def send(e, kinds):
            for kind in kinds:
                core_reduce(e, kind).start()

        half_a, half_b, whole = pl.ds(0, num_local // 2), pl.ds(num_local // 2, num_local // 2), pl.ds(0, num_local)

        def sums_1(e):
            @pl.when(feat >= 0)
            def _():
                put_q(e, q_dot(e, half_a, half_b))
            send(e, (KIND_Q,))

        def sums_2(e):
            @pl.when(feat >= 0)
            def _():
                put_gram(e, KIND_DIAG, gram_dots(KIND_DIAG, whole, half_a, half_b), False)
            send(e, (KIND_VEC, KIND_DIAG))
            stage2_q(e)

            @pl.when(feat >= 0)
            def _():
                put_gram(e, KIND_OFF, gram_dots(KIND_OFF, whole, half_a, half_b), False)
            send(e, (KIND_OFF,))

        for e in range(2):
            pd[e] = jnp.zeros((8, BLK), F32)

        def loop(num, body):
            lax.fori_loop(0, num, lambda t, c: (body(t), c)[1], 0)

        def at(t, when, fn, *args):
            @pl.when(t == when)
            def _():
                fn(*args)

        def par_copy(index):
            src, dst = ((mu_hbm, mu_ref), (lam_hbm, lam_ref), (u_hbm, u_ref))[index]
            return pltpu.make_async_copy(src, dst, par_sem.at[index])

        for c in range(num_tiles):
            in_copy(0, c).start()
        for index in range(3):
            par_copy(index).start()
        barrier = pltpu.get_barrier_semaphore()
        for peer in (peer_core, peer_chip, peer_cross):
            pl.semaphore_signal(barrier, inc=1, device_id=peer, device_id_type=pl.DeviceIdType.MESH)
        def send_gram(e):
            gram(e, KIND_DIAG)
            stage2_q(e)
            gram(e, KIND_OFF)

        for e in range(2):
            pg[e] = jnp.zeros((nblk, grow, BLK), F32)
        def first_pass(c):
            first_chunk(0, c)
            in_copy(1, c).start()
        loop(num_tiles, first_pass)
        par_copy(0).wait()
        par_copy(2).wait()
        pl.semaphore_wait(barrier, 3)
        send(0, (KIND_VEC, KIND_DIAG, KIND_OFF))
        sums_1(0)
        stage2_g(0, KIND_DIAG)

        def second_pass(c):
            first_chunk(1, c)
            at(c, P2Q, stage2_q, 0)
            at(c, P2O, stage2_g, 0, KIND_OFF)
        loop(num_tiles, second_pass)
        send(1, (KIND_VEC, KIND_DIAG, KIND_OFF))
        stage3_q(0)
        stage3_g(0, KIND_DIAG)
        sums_1(1)
        stage3_g(0, KIND_OFF)
        stage4(0, (KIND_Q,))
        stage2_q(1)
        par_copy(1).wait()

        def finish_mix(e, o):
            stage5_q(e)
            stage4(e, (KIND_DIAG,))

            def mix_body(t):
                mix(e, t)
                at(t, T4O, stage4, e, (KIND_OFF, KIND_VEC))
                if o is not None:
                    at(t, T2D, stage2_g, o, KIND_DIAG)
                    at(t, T2O, stage2_g, o, KIND_OFF)
            loop(num_local // MTILE, mix_body)
            stage5(e, KIND_DIAG)
            stage5(e, KIND_OFF)

        def half_step(e):
            o = 1 - e
            finish_mix(e, o)

            def drive_body(t):
                round_inputs(e, tile_ds(t, DTILE), drive(e, tile_ds(t, DTILE)))
                at(t, 0, stage3_q, o)
            loop(num_local // DTILE, drive_body)
            stage3_g(o, KIND_DIAG)
            sums_1(e)
            stage4(o, (KIND_Q,))
            stage3_g(o, KIND_OFF)
            sums_2(e)

        def last_half_step():
            finish_mix(0, 1)

            def drive_body(t):
                drive(0, tile_ds(t, LTILE))
                at(t, 0, stage3_q, 1)
                at(t, L3D, stage3_g, 1, KIND_DIAG)
            loop(num_local // LTILE, drive_body)
            stage3_g(1, KIND_OFF)
            stage4(1, (KIND_Q,))
            finish_mix(1, None)

        def steady(i, carry):
            half_step(i % 2)
            return carry

        lax.fori_loop(0, 2 * (NUM_STEPS - 1), steady, 0)
        last_half_step()

    out_tiles = num_local // OUT_TILE

    def last_kernel(theta, ybuf, kfull, scol, out_hbm, new, out_sem):
        def first(t):
            ds = pl.ds(t * (num_part // out_tiles), num_part // out_tiles)
            return pltpu.make_async_copy(theta.at[0, ds], out_hbm.at[0, ds], out_sem.at[out_tiles + t])

        for t in range(out_tiles):
            first(t).start()

        def out_copy(t):
            ds = pl.ds(pl.multiple_of(t * OUT_TILE, OUT_TILE), OUT_TILE)
            return pltpu.make_async_copy(new.at[:, ds], out_hbm.at[1, :, ds], out_sem.at[t])

        def body(t, carry):
            ds = pl.ds(pl.multiple_of(t * OUT_TILE, OUT_TILE), OUT_TILE)
            moved = jnp.dot(kfull[...], ybuf[:, ds], preferred_element_type=F32)
            new[:, ds] = theta[1, :, ds] * scol[:, 0:1] - moved
            out_copy(t).start()
            return carry

        lax.fori_loop(0, out_tiles, body, 0)
        for t in range(out_tiles):
            first(t).wait()
            out_copy(t).wait()

    def call(particles, target_mean, precision, low_factor):
        vm = pl.BlockSpec(memory_space=pltpu.VMEM)
        hbm = pl.BlockSpec(memory_space=pltpu.HBM)
        scratch = [
            pltpu.VMEM((num_part, num_local), BF16),
            pltpu.VMEM((2, nblk, BLK, BLK), F32),
            pltpu.VMEM((2, nblk, grow, BLK), F32),
            pltpu.VMEM((2, 8, BLK), F32),
            pltpu.VMEM((2, 2, BLK, BLK), F32),
            pltpu.VMEM((2, 2, grow, BLK), F32),
            pltpu.VMEM((2, 8, BLK), F32),
            pltpu.VMEM((2, 2, BLK, BLK), F32),
            pltpu.VMEM((2, 2, grow, BLK), F32),
            pltpu.VMEM((2, 8, BLK), F32),
            pltpu.VMEM((2, BLK, BLK), F32),
            pltpu.VMEM((2, grow, BLK), F32),
            pltpu.VMEM((2, 8, BLK), F32),
            pltpu.VMEM((8, BLK), F32),
            pltpu.VMEM((2, num_part, BLK), BF16),
            pltpu.VMEM((2, nblk, grow, BLK), BF16),
            pltpu.VMEM((2, nblk, 8, BLK), F32),
            pltpu.VMEM((2, num_local), F32),
            pltpu.VMEM((1, num_local), F32),
            pltpu.VMEM((num_local, BLK), BF16),
            pltpu.SemaphoreType.DMA((2, num_tiles)),
            pltpu.SemaphoreType.DMA((3,)),
            pltpu.SemaphoreType.DMA((2, NUM_SEMS)),
            pltpu.SemaphoreType.DMA((2, NUM_SEMS)),
        ]
        state = pl.pallas_call(
            kernel,
            out_shape=(pltpu.VMEM(particles.shape, F32), pltpu.VMEM((num_part, num_local), BF16),
                       pltpu.VMEM((num_part, num_part), BF16), pltpu.VMEM((num_part, BLK), F32)),
            in_specs=[hbm, hbm, hbm, hbm],
            out_specs=(vm, vm, vm, vm),
            scratch_shapes=scratch,
            compiler_params=pltpu.CompilerParams(
                collective_id=0, has_side_effects=True, vmem_limit_bytes=36 * 1024 * 1024),
            cost_estimate=pl.CostEstimate(flops=30 * 10**9, bytes_accessed=18 * 2**20, transcendentals=0),
        )(particles, target_mean, precision[None, :], low_factor)
        return pl.pallas_call(
            last_kernel,
            out_shape=jax.ShapeDtypeStruct(particles.shape, F32),
            in_specs=[vm, vm, vm, vm],
            out_specs=hbm,
            scratch_shapes=[pltpu.VMEM((num_part, num_local), F32), pltpu.SemaphoreType.DMA((2 * out_tiles,))],
            compiler_params=pltpu.CompilerParams(vmem_limit_bytes=10 * 1024 * 1024),
            cost_estimate=pl.CostEstimate(flops=2 * 10**9, bytes_accessed=16 * 2**20, transcendentals=0),
        )(*state)

    return call


def solution(mesh):
    feat_count = mesh.shape["feat"]
    data_spec = P("ens", None, "feat")

    def local_steps(particles, target_mean, precision, low_factor):
        num_part, num_local = particles.shape[1], particles.shape[2]
        call = build_kernel(num_part, num_local, num_local * feat_count)
        return call(particles, target_mean, precision, low_factor)

    return jax.shard_map(
        local_steps, mesh=mesh,
        in_specs=(data_spec, P("ens", "feat"), P(("ens", "feat")), P(("ens", "feat"), None)),
        out_specs=data_spec, check_vma=False)
```

```python
import jax
import jax.numpy as jnp
from jax import lax
from jax.experimental import pallas as pl
from jax.experimental.pallas import tpu as pltpu
from jax.sharding import PartitionSpec as P

NUM_STEPS = 3
BLK = 128
TILE = 1024
OUT_TILE = 512
MTILE = 2048
DTILE = 2048
MIX_TILES = (2048, 2048)
T2D = 0
T4O = 0
T2O = 1
LTILE = 1024
L3D = 2
P2Q = 0
P2O = 0
F32 = jnp.float32
BF16 = jnp.bfloat16
TRANS_B = (((1,), (1,)), ((), ()))

SEM_CORE, SEM_CHIP, SEM_GATHER, SEM_OWN, SEM_FWD = range(5)
KIND_Q, KIND_DIAG, KIND_OFF, KIND_VEC = range(4)
NUM_KINDS = 4
DIRECT = (KIND_DIAG, KIND_OFF, KIND_VEC)
NUM_SEMS = 5 * NUM_KINDS


def build_kernel(num_part, num_local, total_feat):
    nblk = num_part // BLK
    num_tiles = num_local // TILE
    bandwidth = 2.0 * total_feat
    step_size = 0.25 * total_feat
    two_h = 2.0 / bandwidth
    gain = step_size / num_part
    piece = BLK // nblk
    diag_blocks = ((0, 1, True), (2, 3, True), (0, 1, False), (2, 3, False))
    off_blocks = ((0, 2, False), (0, 3, False), (1, 2, False), (1, 3, False))
    blocks = diag_blocks + off_blocks
    grow = piece * len(blocks)
    split = piece * len(diag_blocks)
    spans = {KIND_DIAG: pl.ds(0, split), KIND_OFF: pl.ds(split, grow - split)}

    def kernel(th_hbm, mu_hbm, lam_hbm, u_hbm, theta, ybuf, kfull, scol,
               tb,
               pq, pg, pd, rq, rg, rd, sq, sg, sd, xq, xg, xd, dfull,
               qall, kall, sall,
               mu_ref, lam_ref, u_ref, in_sem, par_sem, send_sem, recv_sem):
        feat = lax.axis_index("feat")
        chip = feat // 2
        core = feat % 2
        own = 2 * core + chip
        peer_core = {"feat": 2 * chip + (1 - core)}
        peer_chip = {"feat": 2 * (1 - chip) + core}
        peer_cross = {"feat": 2 * (1 - chip) + (1 - core)}

        def rcopy(src, dst, e, group, kind, peer):
            idx = group * NUM_KINDS + kind
            return pltpu.make_async_remote_copy(
                src_ref=src, dst_ref=dst, send_sem=send_sem.at[e, idx], recv_sem=recv_sem.at[e, idx],
                device_id=peer, device_id_type=pl.DeviceIdType.MESH)

        def tile_ds(t, size=TILE):
            return pl.ds(pl.multiple_of(t * size, size), size)

        def in_copy(e, t):
            return pltpu.make_async_copy(th_hbm.at[e, :, tile_ds(t)], theta.at[e, :, tile_ds(t)], in_sem.at[e, t])

        def core_reduce(e, kind):
            if kind == KIND_Q:
                src, dst = pq.at[e, pl.ds(2 * (1 - core), 2)], rq.at[e]
            elif kind == KIND_VEC:
                src, dst = pd.at[e], rd.at[e]
            else:
                src, dst = pg.at[e, pl.ds(2 * (1 - core), 2), spans[kind]], rg.at[e, :, spans[kind]]
            return rcopy(src, dst, e, SEM_CORE, kind, peer_core)

        def chip_reduce(e, kind):
            if kind == KIND_Q:
                src, dst = sq.at[e, 1 - chip], xq.at[e]
            elif kind == KIND_VEC:
                src, dst = sd.at[e], xd.at[e]
            else:
                src, dst = sg.at[e, 1 - chip, spans[kind]], xg.at[e, spans[kind]]
            return rcopy(src, dst, e, SEM_CHIP, kind, peer_chip)

        def gather(e, slot, group, kind, peer):
            if kind == KIND_Q:
                ref = qall.at[e, pl.ds(pl.multiple_of(slot * BLK, BLK), BLK)]
            elif kind == KIND_VEC:
                ref = sall.at[e, slot]
            else:
                ref = kall.at[e, slot, spans[kind]]
            return rcopy(ref, ref, e, group, kind, peer)

        def to_chip(e, kind):
            return gather(e, own, SEM_GATHER, kind, peer_chip)

        def to_core(e, kind):
            return gather(e, own, SEM_OWN, kind, peer_core)

        def to_cross(e, kind):
            return gather(e, own, SEM_FWD, kind, peer_cross)

        def start_gather(e, kind):
            to_chip(e, kind).start()
            if kind in DIRECT:
                to_cross(e, kind).start()
            to_core(e, kind).start()

        def forward(e, kind):
            return gather(e, 2 * core + (1 - chip), SEM_FWD, kind, peer_core)

        def stage2_q(e):
            core_reduce(e, KIND_Q).wait()
            for c in range(2):
                sq[e, c] = pq[e, 2 * core + c] + rq[e, c]
            chip_reduce(e, KIND_Q).start()

        def stage2_g(e, kind):
            if kind == KIND_DIAG:
                core_reduce(e, KIND_VEC).wait()
                sd[e] = pd[e] + rd[e]
                chip_reduce(e, KIND_VEC).start()
            core_reduce(e, kind).wait()
            for c in range(2):
                sg[e, c, spans[kind], :] = pg[e, 2 * core + c, spans[kind], :] + rg[e, c, spans[kind], :]
            chip_reduce(e, kind).start()

        def stage3_q(e):
            chip_reduce(e, KIND_Q).wait()
            full = sq[e, chip] + xq[e]
            qall[e, pl.ds(pl.multiple_of(own * BLK, BLK), BLK), :] = full.astype(BF16)
            start_gather(e, KIND_Q)

        def kernel_of(norm, value):
            return jnp.exp(-jnp.maximum(norm - 2.0 * value, 0.0) / bandwidth)

        def kernel_diag(b):
            norm = dfull[b:b + 1, :]
            return kernel_of(norm + norm, norm)

        def stage3_g(e, kind):
            if kind == KIND_DIAG:
                chip_reduce(e, KIND_VEC).wait()
                dfull[...] = sd[e] + xd[e]
                first, last = 0, len(diag_blocks)
            else:
                first, last = len(diag_blocks), len(blocks)
            chip_reduce(e, kind).wait()
            row_id = lax.broadcasted_iota(jnp.int32, (piece, BLK), 0) + own * piece
            col_id = lax.broadcasted_iota(jnp.int32, (piece, BLK), 1)
            mine = row_id == col_id
            upper, lower = row_id < col_id, row_id > col_id
            diag_cols = {}
            col_sums = [None] * nblk

            def diag_row(b):
                return dfull[b:b + 1, :]

            def diag_col(b):
                if b not in diag_cols:
                    diag_cols[b] = jnp.sum(jnp.where(mine, diag_row(b), 0.0), axis=1, keepdims=True)
                return diag_cols[b]

            def add(b, term):
                col_sums[b] = term if col_sums[b] is None else col_sums[b] + term

            def add_rows(b, term):
                add(b, jnp.where(mine, jnp.sum(term, axis=1, keepdims=True), 0.0))

            for index in range(first, last):
                i, j, packed = blocks[index]
                rows = slice(index * piece, (index + 1) * piece)
                gram_rows = sg[e, chip, rows, :] + xg[e, rows, :]
                if packed:
                    norm = jnp.where(lower, diag_col(j) + diag_row(j), diag_col(i) + diag_row(i))
                else:
                    norm = diag_col(i) + diag_row(j)
                kern = kernel_of(norm, gram_rows)
                kall[e, own, rows, :] = (kern * gain).astype(BF16)
                if packed:
                    kern_up, kern_low = jnp.where(upper, kern, 0.0), jnp.where(lower, kern, 0.0)
                    add(i, jnp.where(lower, 0.0, kern))
                    add_rows(i, kern_up)
                    add(j, kern_low + jnp.where(mine, kernel_diag(j), 0.0))
                    add_rows(j, kern_low)
                else:
                    add(j, kern)
                    add_rows(i, kern)
            for b in range(nblk):
                total = jnp.sum(col_sums[b], axis=0, keepdims=True)
                if kind == KIND_OFF:
                    total = total + sall[e, own, b:b + 1, :]
                sall[e, own, b:b + 1, :] = total
            for k in (kind,) if kind == KIND_DIAG else (kind, KIND_VEC):
                start_gather(e, k)

        def stage4(e, kinds):
            for kind in kinds:
                if kind not in DIRECT:
                    to_chip(e, kind).wait()
                    forward(e, kind).start()

        def arrived(e, kind):
            to_core(e, kind).wait()
            if kind in DIRECT:
                to_chip(e, kind).wait()
                to_cross(e, kind).wait()
            else:
                forward(e, kind).wait()

        def stage5_q(e):
            arrived(e, KIND_Q)

        def stage5(e, kind):
            arrived(e, kind)
            row_id = lax.broadcasted_iota(jnp.int32, (BLK, BLK), 0)
            col_id = lax.broadcasted_iota(jnp.int32, (BLK, BLK), 1)

            def put(i, j, value):
                kfull[i * BLK:(i + 1) * BLK, j * BLK:(j + 1) * BLK] = value.astype(BF16)

            for index, (i, j, packed) in enumerate(blocks):
                if (index < len(diag_blocks)) != (kind == KIND_DIAG):
                    continue
                rows = slice(index * piece, (index + 1) * piece)
                if packed:
                    block = jnp.concatenate([kall[e, o, rows, :].astype(F32) for o in range(nblk)], axis=0)
                    flipped = block.T
                    put(i, i, jnp.where(row_id <= col_id, block, flipped))
                    rest = jnp.where(row_id < col_id, flipped, (kernel_diag(j) * gain).astype(BF16).astype(F32))
                    put(j, j, jnp.where(row_id > col_id, block, rest))
                else:
                    block = jnp.concatenate([kall[e, o, rows, :] for o in range(nblk)], axis=0)
                    put(i, j, block)
                    put(j, i, block.T)
            if kind == KIND_OFF:
                arrived(e, KIND_VEC)
                srow = sall[e, 0] + sall[e, 1] + sall[e, 2] + sall[e, 3]
                eye = (lax.broadcasted_iota(jnp.int32, (BLK, BLK), 0) == lax.broadcasted_iota(jnp.int32, (BLK, BLK), 1))
                for i in range(nblk):
                    col = jnp.sum(jnp.where(eye, srow[i:i + 1, :], 0.0), axis=1, keepdims=True)
                    scol[i * BLK:(i + 1) * BLK, :] = 1.0 + jnp.broadcast_to(col, (BLK, BLK)) * (gain * two_h)

        def round_inputs(e, ds, value):
            tb[:, ds] = value.astype(BF16)

        def mix(e, ds):
            value = theta[e, :, ds]
            low = lax.dot_general(qall[e], u_ref[ds, :], TRANS_B, preferred_element_type=F32)
            centered = value - mu_ref[pl.ds(e, 1), ds]
            ybuf[:, ds] = (centered * (lam_ref[:, ds] + two_h) + (low + two_h * mu_ref[pl.ds(e, 1), ds])).astype(BF16)

        def drive(e, ds):
            moved = jnp.dot(kfull[...], ybuf[:, ds], preferred_element_type=F32)
            new = theta[e, :, ds] * scol[:, 0:1] - moved
            theta[e, :, ds] = new
            return new

        def q_dot(e, ds_a, ds_b):
            parts = [jnp.dot((theta[e, :, d] - mu_ref[pl.ds(e, 1), d]).astype(BF16), u_ref[d, :], preferred_element_type=F32) for d in (ds_a, ds_b)]
            return parts[0] + parts[1]

        def gram_dots(kind, ds_all, ds_a, ds_b):
            two = 2 * BLK
            out = {}
            if kind == KIND_DIAG:
                for half in range(2):
                    rows = tb[half * two:(half + 1) * two, ds_all]
                    prod = lax.dot_general(rows, rows, TRANS_B, preferred_element_type=F32)
                    for i in range(2):
                        for j in range(i, 2):
                            out[2 * half + i, 2 * half + j] = prod[i * BLK:(i + 1) * BLK, j * BLK:(j + 1) * BLK]
            else:
                prod = [lax.dot_general(tb[0:two, d], tb[two:2 * two, d], TRANS_B, preferred_element_type=F32)
                        for d in (ds_a, ds_b)]
                prod = prod[0] + prod[1]
                for i in range(2):
                    for j in range(2):
                        out[i, 2 + j] = prod[i * BLK:(i + 1) * BLK, j * BLK:(j + 1) * BLK]
            return out

        def put_q(e, value):
            for i in range(nblk):
                pq[e, i] = value[i * BLK:(i + 1) * BLK, :]

        def put_gram(e, kind, out, add):
            row_id = lax.broadcasted_iota(jnp.int32, (BLK, BLK), 0)
            col_id = lax.broadcasted_iota(jnp.int32, (BLK, BLK), 1)
            for index, (i, j, packed) in enumerate(blocks):
                if (index < len(diag_blocks)) != (kind == KIND_DIAG):
                    continue
                block = jnp.where(row_id <= col_id, out[i, i], out[j, j]) if packed else out[i, j]
                for o in range(nblk):
                    rows = slice(index * piece, (index + 1) * piece)
                    term = block[o * piece:(o + 1) * piece]
                    pg[e, o, rows, :] = pg[e, o, rows, :] + term if add else term
            if kind == KIND_DIAG:
                for i in range(nblk):
                    term = jnp.sum(jnp.where(row_id == col_id, out[i, i], 0.0), axis=0, keepdims=True)
                    pd[e, i:i + 1, :] = pd[e, i:i + 1, :] + term if add else term

        def first_chunk(e, c):
            half = TILE // 2
            in_copy(e, c).wait()
            round_inputs(e, tile_ds(c), theta[e, :, tile_ds(c)])
            start = pl.multiple_of(c * TILE, TILE)
            ds_a, ds_b = pl.ds(start, half), pl.ds(start + half, half)
            for kind in (KIND_DIAG, KIND_OFF):
                put_gram(e, kind, gram_dots(kind, tile_ds(c), ds_a, ds_b), True)

        def send(e, kinds):
            for kind in kinds:
                core_reduce(e, kind).start()

        half_a, half_b, whole = pl.ds(0, num_local // 2), pl.ds(num_local // 2, num_local // 2), pl.ds(0, num_local)

        def sums_1(e):
            @pl.when(feat >= 0)
            def _():
                put_q(e, q_dot(e, half_a, half_b))
            send(e, (KIND_Q,))

        def sums_2(e):
            @pl.when(feat >= 0)
            def _():
                put_gram(e, KIND_DIAG, gram_dots(KIND_DIAG, whole, half_a, half_b), False)
            send(e, (KIND_VEC, KIND_DIAG))
            stage2_q(e)

            @pl.when(feat >= 0)
            def _():
                put_gram(e, KIND_OFF, gram_dots(KIND_OFF, whole, half_a, half_b), False)
            send(e, (KIND_OFF,))

        for e in range(2):
            pd[e] = jnp.zeros((8, BLK), F32)

        def loop(num, body):
            lax.fori_loop(0, num, lambda t, c: (body(t), c)[1], 0)

        def at(t, when, fn, *args):
            @pl.when(t == when)
            def _():
                fn(*args)

        def par_copy(index):
            src, dst = ((mu_hbm, mu_ref), (lam_hbm, lam_ref), (u_hbm, u_ref))[index]
            return pltpu.make_async_copy(src, dst, par_sem.at[index])

        for c in range(num_tiles):
            in_copy(0, c).start()
        for index in range(3):
            par_copy(index).start()
        barrier = pltpu.get_barrier_semaphore()
        for peer in (peer_core, peer_chip, peer_cross):
            pl.semaphore_signal(barrier, inc=1, device_id=peer, device_id_type=pl.DeviceIdType.MESH)
        def send_gram(e):
            gram(e, KIND_DIAG)
            stage2_q(e)
            gram(e, KIND_OFF)

        for e in range(2):
            pg[e] = jnp.zeros((nblk, grow, BLK), F32)
        def first_pass(c):
            first_chunk(0, c)
            in_copy(1, c).start()
        loop(num_tiles, first_pass)
        par_copy(0).wait()
        par_copy(2).wait()
        pl.semaphore_wait(barrier, 3)
        send(0, (KIND_VEC, KIND_DIAG, KIND_OFF))
        sums_1(0)
        stage2_g(0, KIND_DIAG)

        def second_pass(c):
            first_chunk(1, c)
            at(c, P2Q, stage2_q, 0)
            at(c, P2O, stage2_g, 0, KIND_OFF)
        loop(num_tiles, second_pass)
        send(1, (KIND_VEC, KIND_DIAG, KIND_OFF))
        stage3_q(0)
        stage3_g(0, KIND_DIAG)
        sums_1(1)
        stage3_g(0, KIND_OFF)
        stage4(0, (KIND_Q,))
        stage2_q(1)
        par_copy(1).wait()

        def finish_mix(e, o):
            stage5_q(e)
            stage4(e, (KIND_DIAG,))

            start = 0
            for t, size in enumerate(MIX_TILES):
                @pl.when(feat >= 0)
                def _():
                    mix(e, pl.ds(start, size))
                start += size
                if t == T4O:
                    stage4(e, (KIND_OFF, KIND_VEC))
                if o is not None and t == T2D:
                    stage2_g(o, KIND_DIAG)
                if o is not None and t == T2O:
                    stage2_g(o, KIND_OFF)
            stage5(e, KIND_DIAG)
            stage5(e, KIND_OFF)

        def half_step(e):
            o = 1 - e
            finish_mix(e, o)

            def drive_body(t):
                round_inputs(e, tile_ds(t, DTILE), drive(e, tile_ds(t, DTILE)))
                at(t, 0, stage3_q, o)
            loop(num_local // DTILE, drive_body)
            stage3_g(o, KIND_DIAG)
            sums_1(e)
            stage3_g(o, KIND_OFF)
            stage4(o, (KIND_Q,))
            sums_2(e)

        def last_half_step():
            finish_mix(0, 1)

            def drive_body(t):
                drive(0, tile_ds(t, LTILE))
                at(t, 0, stage3_q, 1)
                at(t, L3D, stage3_g, 1, KIND_DIAG)
            loop(num_local // LTILE, drive_body)
            stage3_g(1, KIND_OFF)
            stage4(1, (KIND_Q,))
            finish_mix(1, None)

        def steady(i, carry):
            half_step(i % 2)
            return carry

        lax.fori_loop(0, 2 * (NUM_STEPS - 1), steady, 0)
        last_half_step()

    out_tiles = num_local // OUT_TILE

    def last_kernel(theta, ybuf, kfull, scol, out_hbm, new, out_sem):
        def first(t):
            ds = pl.ds(t * (num_part // out_tiles), num_part // out_tiles)
            return pltpu.make_async_copy(theta.at[0, ds], out_hbm.at[0, ds], out_sem.at[out_tiles + t])

        for t in range(out_tiles):
            first(t).start()

        def out_copy(t):
            ds = pl.ds(pl.multiple_of(t * OUT_TILE, OUT_TILE), OUT_TILE)
            return pltpu.make_async_copy(new.at[:, ds], out_hbm.at[1, :, ds], out_sem.at[t])

        def body(t, carry):
            ds = pl.ds(pl.multiple_of(t * OUT_TILE, OUT_TILE), OUT_TILE)
            moved = jnp.dot(kfull[...], ybuf[:, ds], preferred_element_type=F32)
            new[:, ds] = theta[1, :, ds] * scol[:, 0:1] - moved
            out_copy(t).start()
            return carry

        lax.fori_loop(0, out_tiles, body, 0)
        for t in range(out_tiles):
            first(t).wait()
            out_copy(t).wait()

    def call(particles, target_mean, precision, low_factor):
        vm = pl.BlockSpec(memory_space=pltpu.VMEM)
        hbm = pl.BlockSpec(memory_space=pltpu.HBM)
        scratch = [
            pltpu.VMEM((num_part, num_local), BF16),
            pltpu.VMEM((2, nblk, BLK, BLK), F32),
            pltpu.VMEM((2, nblk, grow, BLK), F32),
            pltpu.VMEM((2, 8, BLK), F32),
            pltpu.VMEM((2, 2, BLK, BLK), F32),
            pltpu.VMEM((2, 2, grow, BLK), F32),
            pltpu.VMEM((2, 8, BLK), F32),
            pltpu.VMEM((2, 2, BLK, BLK), F32),
            pltpu.VMEM((2, 2, grow, BLK), F32),
            pltpu.VMEM((2, 8, BLK), F32),
            pltpu.VMEM((2, BLK, BLK), F32),
            pltpu.VMEM((2, grow, BLK), F32),
            pltpu.VMEM((2, 8, BLK), F32),
            pltpu.VMEM((8, BLK), F32),
            pltpu.VMEM((2, num_part, BLK), BF16),
            pltpu.VMEM((2, nblk, grow, BLK), BF16),
            pltpu.VMEM((2, nblk, 8, BLK), F32),
            pltpu.VMEM((2, num_local), F32),
            pltpu.VMEM((1, num_local), F32),
            pltpu.VMEM((num_local, BLK), BF16),
            pltpu.SemaphoreType.DMA((2, num_tiles)),
            pltpu.SemaphoreType.DMA((3,)),
            pltpu.SemaphoreType.DMA((2, NUM_SEMS)),
            pltpu.SemaphoreType.DMA((2, NUM_SEMS)),
        ]
        state = pl.pallas_call(
            kernel,
            out_shape=(pltpu.VMEM(particles.shape, F32), pltpu.VMEM((num_part, num_local), BF16),
                       pltpu.VMEM((num_part, num_part), BF16), pltpu.VMEM((num_part, BLK), F32)),
            in_specs=[hbm, hbm, hbm, hbm],
            out_specs=(vm, vm, vm, vm),
            scratch_shapes=scratch,
            compiler_params=pltpu.CompilerParams(
                collective_id=0, has_side_effects=True, vmem_limit_bytes=36 * 1024 * 1024),
            cost_estimate=pl.CostEstimate(flops=30 * 10**9, bytes_accessed=18 * 2**20, transcendentals=0),
        )(particles, target_mean, precision[None, :], low_factor)
        return pl.pallas_call(
            last_kernel,
            out_shape=jax.ShapeDtypeStruct(particles.shape, F32),
            in_specs=[vm, vm, vm, vm],
            out_specs=hbm,
            scratch_shapes=[pltpu.VMEM((num_part, num_local), F32), pltpu.SemaphoreType.DMA((2 * out_tiles,))],
            compiler_params=pltpu.CompilerParams(vmem_limit_bytes=10 * 1024 * 1024),
            cost_estimate=pl.CostEstimate(flops=2 * 10**9, bytes_accessed=16 * 2**20, transcendentals=0),
        )(*state)

    return call


def solution(mesh):
    feat_count = mesh.shape["feat"]
    data_spec = P("ens", None, "feat")

    def local_steps(particles, target_mean, precision, low_factor):
        num_part, num_local = particles.shape[1], particles.shape[2]
        call = build_kernel(num_part, num_local, num_local * feat_count)
        return call(particles, target_mean, precision, low_factor)

    return jax.shard_map(
        local_steps, mesh=mesh,
        in_specs=(data_spec, P("ens", "feat"), P(("ens", "feat")), P(("ens", "feat"), None)),
        out_specs=data_spec, check_vma=False)
```
